32 devices in a mesh: seq: 4 (over y, core), head: 4 (over z), batch: 2 (over x).
Axes of the slice: x: 2, y: 2, z: 4, core: 2. Of those that a mesh axis runs over, the one named last changes fastest.
Arguments:
- query_vectors: bfloat16 [4, 4096, 2048], P('batch', 'seq', 'head'), parts along dimension 0, may hold values from -6 to 6
- key_vectors: bfloat16 [4, 4096, 2048], P('batch', 'seq', 'head'), parts along dimension 0, may hold values from -6 to 6
- value_vectors: bfloat16 [4, 4096, 2048], P('batch', 'seq', 'head'), parts along dimension 0, may hold values from -6 to 6
- token_rates: float32 [4, 16, 4096], P('batch', 'head', 'seq'), parts along dimension 0, may hold values from 0.05 to 1
- gate_weight: float32 [16, 128, 256], P('head'), may hold values from -0.5 to 0.5
- up_weight: float32 [16, 128, 256], P('head'), may hold values from -0.5 to 0.5
- down_weight: float32 [16, 128, 256], P('head'), may hold values from -0.375 to 0.375
- step_sizes: float32 [16], P('head'), may hold values from 0.3 to 1
- norm_gain: float32 [2048], P('head'), may hold values from 0.1 to 1.9
Outputs:
- mixed: bfloat16 [4, 4096, 2048], P('batch', 'seq', 'head'), parts along dimension 0
- final_weights: float32 [6, 16, 128, 256], P('batch', 'head'), parts along dimension 0
The draws below stay inside these ranges and needn't reach their ends.
There are 2 independent parts, one for each index of `batch`. The reference program is written for one: setup_inputs(seed, part) draws one part's arguments, and reference() takes and returns one part's arrays. A program takes and returns all parts, laid end to end along the dimension named above; an argument that names none is the same for every part. Nothing has to cross between parts.
All inputs are finite; a program needn't handle non-finite values.
Results may differ from the reference program's by a relative error of at most 0.008.
Values may be sent and summed in bfloat16 or wider, within the bound.
A program may use at most 128 MiB of HBM per device.

```python
import math
import jax
import jax.numpy as jnp
from jax import lax

HD = 128
FW = 256
HEADS = 16
TOK_DEV = 1024
GROUPS = 2
NS_STEPS = 5
GROUP = 4096
WINDOW = 2048


def drawn_pair(key):
    shape = (GROUPS, GROUP, HEADS * HD)
    first, second = jax.random.split(jax.random.fold_in(key, 4242), 2)
    query_draw = jax.random.truncated_normal(first, -5.5, 5.5, shape, jnp.float32)
    key_draw = jax.random.truncated_normal(second, -5.5, 5.5, shape, jnp.float32)
    return (query_draw.astype(jnp.bfloat16), key_draw.astype(jnp.bfloat16))


def draw_query_vectors(key, part):
    return drawn_pair(key)[0]


def draw_key_vectors(key, part):
    return drawn_pair(key)[1]


def level_of(key, dims, shards, least, top_value):
    factor_of, own = 1.0, jax.random.fold_in(key, 6)
    for axis_at, shards_of in shards:
        draws = jnp.exp(jax.random.uniform(jax.random.fold_in(own, axis_at), (shards_of,), jnp.float32, least / len(shards), top_value / len(shards)))
        factor_of = factor_of * jnp.repeat(draws, dims[axis_at] // shards_of).reshape([-1 if axis == axis_at else 1 for axis in range(len(dims))])
    return factor_of


def scatter_about(key, shape, scale, most, shards=(), held_as=jnp.bfloat16):
    factor_of = level_of(key, shape, shards, -0.22, 0.18) if shards else 1.0
    entries = jax.random.normal(key, shape, jnp.float32) * scale * factor_of
    return jnp.minimum(jnp.maximum(entries, -most), most).astype(held_as)


def setup_inputs(seed: int = 0, part: int = 0) -> dict:
    key_of = jax.random.split(jax.random.key(seed), 10)
    own_keys = jax.random.split(jax.random.fold_in(key_of[9], part), 10)
    query_vectors = draw_query_vectors(jax.random.fold_in(jax.random.fold_in(key_of[9], part), 71), part)
    key_vectors = draw_key_vectors(jax.random.fold_in(jax.random.fold_in(key_of[9], part), 71), part)
    value_vectors = scatter_about(own_keys[2], (GROUPS, GROUP, HEADS * HD), 1.0, 6.0, ((1, 4), (2, 4)))
    token_rates = jnp.clip(jnp.exp(math.log(1.0) - 2.9957323 * jax.random.uniform(own_keys[3], (GROUPS, HEADS, GROUP), jnp.float32) ** level_of(own_keys[3], (GROUPS, HEADS, GROUP), ((1, 4), (2, 4)), -0.2, 0.2)), 0.05, 1.0)
    gate_weight = scatter_about(key_of[4], (HEADS, HD, FW), HD ** -0.5, 0.5, ((0, 4),), jnp.float32)
    up_weight = scatter_about(key_of[5], (HEADS, HD, FW), HD ** -0.5, 0.5, ((0, 4),), jnp.float32)
    down_weight = scatter_about(key_of[6], (HEADS, HD, FW), FW ** -0.5, 0.375, ((0, 4),), jnp.float32)
    step_sizes = jnp.clip(jnp.exp(math.log(1.0) - 1.2039728 * jax.random.uniform(key_of[7], (HEADS,), jnp.float32) ** level_of(key_of[7], (HEADS,), ((0, 4),), -0.2, 0.2)), 0.3, 1.0)
    norm_gain = jnp.clip(1.0 + 0.18 * jax.random.normal(key_of[8], (HEADS * HD,), jnp.float32), 0.1, 1.9)
    return {"query_vectors": query_vectors, "key_vectors": key_vectors, "value_vectors": value_vectors, "token_rates": token_rates, "gate_weight": gate_weight, "up_weight": up_weight, "down_weight": down_weight, "step_sizes": step_sizes, "norm_gain": norm_gain}


coeff_first = 3.4445
coeff_second = -4.775
coeff_third = 2.0315
frob_epsilon = 1e-07
rms_epsilon = 1e-06
column_epsilon = 1e-06

def fast_forward(inputs, w_gate, w_up):
    gate_pre = jnp.dot(inputs, w_gate.astype(jnp.bfloat16), preferred_element_type=jnp.float32)
    up_pre = jnp.dot(inputs, w_up.astype(jnp.bfloat16), preferred_element_type=jnp.float32)
    squash = jax.nn.sigmoid(gate_pre)
    active = gate_pre * squash
    hidden_act = (active * up_pre).astype(jnp.bfloat16)
    return (gate_pre, up_pre, squash, active, hidden_act)

def fast_apply(items):
    queries, w_gate, w_up, w_down = items
    hidden_act = fast_forward(queries, w_gate, w_up)[4]
    return jnp.dot(hidden_act, w_down.astype(jnp.bfloat16).T, preferred_element_type=jnp.float32)

def fast_grads(items):
    key_rows, value_rows, rate_rows, w_gate, w_up, w_down = items
    gate_pre, up_pre, squash, active, hidden_act = fast_forward(key_rows, w_gate, w_up)
    out_grad = (-rate_rows[:, None] * value_rows.astype(jnp.float32)).astype(jnp.bfloat16)
    grad_down = jnp.dot(out_grad.T, hidden_act, preferred_element_type=jnp.float32)
    hidden_grad = jnp.dot(out_grad, w_down.astype(jnp.bfloat16), preferred_element_type=jnp.float32)
    up_grad = (hidden_grad * active).astype(jnp.bfloat16)
    gate_grad = (hidden_grad * up_pre * squash * (1.0 + gate_pre * (1.0 - squash))).astype(jnp.bfloat16)
    grad_gate = jnp.dot(key_rows.T, gate_grad, preferred_element_type=jnp.float32)
    grad_up = jnp.dot(key_rows.T, up_grad, preferred_element_type=jnp.float32)
    return (grad_gate, grad_up, grad_down)

def orthogonalize(gradient):
    matrix = gradient / (jnp.sqrt(jnp.sum(gradient * gradient)) + frob_epsilon)
    for sweep in range(NS_STEPS):
        gram_matrix = jnp.dot(matrix, matrix.T, precision=lax.Precision.HIGHEST)
        polynomial = coeff_second * gram_matrix + coeff_third * jnp.dot(gram_matrix, gram_matrix, precision=lax.Precision.HIGHEST)
        matrix = coeff_first * matrix + jnp.dot(polynomial, matrix, precision=lax.Precision.HIGHEST)
    return matrix

def renew(weight, gradient, step_rate, target):
    stepped = weight - step_rate * orthogonalize(gradient)
    length = jnp.sqrt(lax.optimization_barrier(jnp.sum(stepped * stepped, axis=0)))
    return stepped * (target / (length + column_epsilon))

def window_attention(queries, key_rows, value_rows):
    row_count = queries.shape[0]
    block_rows = min(512, TOK_DEV)
    scale = 1.0 / math.sqrt(HD)
    front_pad = jnp.zeros((WINDOW, HEADS, HD), jnp.bfloat16)
    keys_padded = jnp.concatenate([front_pad, key_rows], axis=0)
    values_padded = jnp.concatenate([front_pad, value_rows], axis=0)

    def one_block(block_index):
        first_row = (block_index * block_rows).astype(jnp.int32)
        query_block = lax.dynamic_slice_in_dim(queries, first_row, block_rows, 0).astype(jnp.float32)
        key_block = lax.dynamic_slice_in_dim(keys_padded, first_row, WINDOW + block_rows, 0).astype(jnp.float32)
        value_block = lax.dynamic_slice_in_dim(values_padded, first_row, WINDOW + block_rows, 0).astype(jnp.float32)
        scores = jnp.einsum('qhd,khd->hqk', query_block, key_block) * scale
        offset = jnp.arange(block_rows, dtype=jnp.int32)[:, None] - jnp.arange(WINDOW + block_rows, dtype=jnp.int32)[None, :] + WINDOW
        key_place = first_row - WINDOW + jnp.arange(WINDOW + block_rows, dtype=jnp.int32)
        allowed = (offset >= 0) & (offset < WINDOW) & (key_place[None, :] >= 0)
        scores = jnp.where(allowed[None], scores, -jnp.inf)
        row_max = lax.optimization_barrier(jnp.max(scores, axis=-1, keepdims=True))
        raised = jnp.exp(scores - row_max)
        attend = (raised / lax.optimization_barrier(jnp.sum(raised, axis=-1, keepdims=True))).astype(jnp.bfloat16)
        return jnp.einsum('hqk,khd->qhd', attend.astype(jnp.float32), value_block)
    blocks_out = lax.map(one_block, jnp.arange(row_count // block_rows, dtype=jnp.int32))
    return blocks_out.reshape(row_count, HEADS, HD)

def reference(query_vectors, key_vectors, value_vectors, token_rates, gate_weight, up_weight, down_weight, step_sizes, norm_gain):
    attended = window_attention(query_vectors.reshape(GROUPS * GROUP, HEADS, HD), key_vectors.reshape(GROUPS * GROUP, HEADS, HD), value_vectors.reshape(GROUPS * GROUP, HEADS, HD))
    attended = attended.reshape(GROUPS, GROUP, HEADS, HD)
    weights = (gate_weight, up_weight, down_weight)
    targets = tuple((jnp.sqrt(lax.optimization_barrier(jnp.sum(matrix_in * matrix_in, axis=1))) for matrix_in in weights))
    gain = norm_gain.reshape(HEADS, HD)
    mixed_groups = []
    for group in range(GROUPS):
        query_group = query_vectors[group].reshape(GROUP, HEADS, HD).transpose(1, 0, 2)
        key_group = key_vectors[group].reshape(GROUP, HEADS, HD).transpose(1, 0, 2)
        value_group = value_vectors[group].reshape(GROUP, HEADS, HD).transpose(1, 0, 2)
        applied = lax.map(fast_apply, (query_group,) + weights).transpose(1, 0, 2)
        normed = applied * lax.rsqrt(lax.optimization_barrier(jnp.mean(applied * applied, axis=-1, keepdims=True)) + rms_epsilon) * gain
        mixed_groups.append((normed + attended[group]).astype(jnp.bfloat16).reshape(GROUP, HEADS * HD))
        gradients = lax.map(fast_grads, (key_group, value_group, token_rates[group]) + weights)
        weights = tuple((jax.vmap(renew)(weights[which], gradients[which], step_sizes, targets[which]) for which in range(3)))
    return (jnp.stack(mixed_groups), jnp.stack(weights))
```

```python
import functools
import math

import jax
import jax.numpy as jnp
from jax import lax
from jax.experimental import pallas as pl
from jax.experimental.pallas import tpu as pltpu
from jax.sharding import PartitionSpec as P

HD = 128
NS_STEPS = 5

coeff_first = 3.4445
coeff_second = -4.775
coeff_third = 2.0315
frob_epsilon = 1e-07
rms_epsilon = 1e-06
column_epsilon = 1e-06
EXCLUDED = -1e30
BARRED = -3e30
VMEM_GRANT = 58 * 2**20


def dot(a, b, dims):
    return lax.dot_general(a, b, (dims, ((), ())), preferred_element_type=jnp.float32)


def sigmoid(a):
    return 0.5 * jnp.tanh(0.5 * a) + 0.5


def grads_kernel(chunk, key_ref, value_ref, rate_ref, weight_ref, out_ref):
    head = pl.program_id(0)
    width = weight_ref.shape[-1]
    rows = key_ref.shape[0]
    gate_up = jnp.concatenate([weight_ref[0], weight_ref[1]], axis=1).astype(jnp.bfloat16)
    down = weight_ref[2].astype(jnp.bfloat16)
    for start in range(0, rows, chunk):
        part = pl.ds(start, chunk)
        keys = key_ref[part, :]
        rates = rate_ref[part, :]
        lane = lax.broadcasted_iota(jnp.int32, rates.shape, 1)
        rate = jnp.sum(jnp.where(lane == head, rates, 0.0), axis=1, keepdims=True)
        out_grad = (-rate * value_ref[part, :].astype(jnp.float32)).astype(jnp.bfloat16)
        pre = dot(keys, gate_up, ((1,), (0,)))
        gate_pre, up_pre = pre[:, :width], pre[:, width:]
        squash = sigmoid(gate_pre)
        active = gate_pre * squash
        hidden = (active * up_pre).astype(jnp.bfloat16)
        hidden_grad = dot(out_grad, down, ((1,), (0,)))
        up_grad = (hidden_grad * active).astype(jnp.bfloat16)
        gate_grad = (hidden_grad * up_pre * squash * (1.0 + gate_pre * (1.0 - squash))).astype(
            jnp.bfloat16
        )
        terms = (
            dot(keys, gate_grad, ((0,), (0,))),
            dot(keys, up_grad, ((0,), (0,))),
            dot(out_grad, hidden, ((0,), (0,))),
        )
        for which in range(3):
            if start == 0:
                out_ref[which] = terms[which]
            else:
                out_ref[which] += terms[which]


def group_gradients(group, keys, values, rates, weights):
    _, rows, features = keys.shape
    heads = features // HD
    width = weights.shape[-1]
    token_spec = pl.BlockSpec((None, rows, HD), lambda h: (group, 0, h))
    return pl.pallas_call(
        functools.partial(grads_kernel, min(256, rows)),
        grid=(heads,),
        in_specs=[
            token_spec,
            token_spec,
            pl.BlockSpec((None, rows, heads), lambda h: (group, 0, 0)),
            pl.BlockSpec((None, 3, HD, width), lambda h: (h, 0, 0, 0)),
        ],
        out_specs=pl.BlockSpec((None, 3, HD, width), lambda h: (h, 0, 0, 0)),
        out_shape=jax.ShapeDtypeStruct((heads, 3, HD, width), jnp.float32),
        cost_estimate=pl.CostEstimate(
            flops=6 * 2 * 2 * heads * rows * HD * width,
            bytes_accessed=2 * rows * features * 2 + heads * 3 * HD * width * 8,
            transcendentals=heads * rows * width,
        ),
        name="group_gradients",
    )(keys, values, rates, weights)


def split(a):
    high = a.astype(jnp.bfloat16)
    return high, (a - high.astype(jnp.float32)).astype(jnp.bfloat16)


def renew_kernel(parts, *refs):
    grad_refs = refs[:parts]
    first_ref, weight_ref, step_ref, new_ref, low_ref = refs[parts:]
    step = step_ref[pl.program_id(0)]
    matrices = []
    for which in range(3):
        gradient = grad_refs[0][which]
        for ref in grad_refs[1:]:
            gradient = gradient + ref[which]
        frobenius = jnp.sqrt(jnp.sum(gradient * gradient, keepdims=True))
        matrices.append(gradient / (frobenius + frob_epsilon))
    for sweep in range(NS_STEPS):
        pairs = [split(matrix) for matrix in matrices]
        grams = [
            dot(
                jnp.concatenate([high, high, rest], axis=1),
                jnp.concatenate([high, rest, high], axis=1),
                ((1,), (1,)),
            )
            for high, rest in pairs
        ]
        polynomials = []
        for gram in grams:
            high, rest = split(gram)
            squared = dot(
                jnp.concatenate([high, high, rest], axis=1),
                jnp.concatenate([high, rest, high], axis=0),
                ((1,), (0,)),
            )
            polynomials.append(coeff_second * gram + coeff_third * squared)
        moved = []
        for polynomial, (high, rest), matrix in zip(polynomials, pairs, matrices):
            poly_high, poly_rest = split(polynomial)
            moved.append(
                coeff_first * matrix
                + dot(
                    jnp.concatenate([poly_high, poly_high, poly_rest], axis=1),
                    jnp.concatenate([high, rest, high], axis=0),
                    ((1,), (0,)),
                )
            )
        matrices = moved
    for which in range(3):
        first = first_ref[which]
        target = jnp.sqrt(jnp.sum(first * first, axis=0, keepdims=True))
        stepped = weight_ref[which] - step * matrices[which]
        length = jnp.sqrt(jnp.sum(stepped * stepped, axis=0, keepdims=True))
        renewed = stepped * (target / (length + column_epsilon))
        new_ref[which] = renewed
        low_ref[which] = renewed.astype(jnp.bfloat16)


def renew(gradients, first, weights, steps):
    heads, _, _, width = weights.shape
    spec = pl.BlockSpec((None, 3, HD, width), lambda h: (h, 0, 0, 0))
    return pl.pallas_call(
        functools.partial(renew_kernel, len(gradients)),
        grid=(heads,),
        in_specs=[spec] * (len(gradients) + 2) + [pl.BlockSpec(memory_space=pltpu.SMEM)],
        out_specs=[spec, spec],
        out_shape=[
            jax.ShapeDtypeStruct(weights.shape, jnp.float32),
            jax.ShapeDtypeStruct(weights.shape, jnp.bfloat16),
        ],
        cost_estimate=pl.CostEstimate(
            flops=heads * 3 * NS_STEPS * 10 * HD * HD * width * 4,
            bytes_accessed=heads * 3 * HD * width * 20,
            transcendentals=0,
        ),
        name="renew_weights",
    )(*gradients, first, weights, steps)


def mix_kernel(
    tile,
    guarded,
    bias_ref,
    query_ref,
    key_far,
    key_near,
    key_own,
    value_far,
    value_near,
    value_own,
    weight_ref,
    gain_ref,
    *rest,
):
    out_ref, score_ref = rest[-2:]
    rows = query_ref.shape[0]
    width = weight_ref.shape[-1]
    per = rows // tile
    blocks = per
    span = 2 * per + 1
    factor = math.log2(math.e) / math.sqrt(HD)
    key_refs = (key_far, key_near, key_own)
    value_refs = (value_far, value_near, value_own)
    gate_up = jnp.concatenate([weight_ref[0], weight_ref[1]], axis=1).astype(jnp.bfloat16)
    down = weight_ref[2].astype(jnp.bfloat16)
    gain = gain_ref[...]
    row = lax.broadcasted_iota(jnp.int32, (tile, tile), 0)
    column = lax.broadcasted_iota(jnp.int32, (tile, tile), 1)
    later = column > row

    def fold(op, a):
        folded = a[:, :HD]
        for at in range(HD, tile, HD):
            folded = op(folded, a[:, at : at + HD])
        return folded

    def score(block, at, peak):
        source, place = divmod(block + at, per)
        queries = query_ref[block * tile : (block + 1) * tile, :]
        s = dot(queries, key_refs[source][place * tile : (place + 1) * tile, :], ((1,), (1,)))
        if at == 0:
            s = jnp.where(later, s, EXCLUDED)
        if at == span - 1:
            s = jnp.where(later, EXCLUDED, s)
        if guarded and source < 2:
            s = s + bias_ref[source]
        score_ref[block % 2, at] = s
        top = fold(jnp.maximum, s)
        return top if peak is None else jnp.maximum(peak, top)

    peak = None
    for at in range(span):
        peak = score(0, at, peak)
    for block in range(blocks):
        row_max = jnp.max(peak, axis=1, keepdims=True)
        peak = None
        total = None
        summed = None
        for at in range(span):
            if block + 1 < blocks:
                peak = score(block + 1, at, peak)
            raised = jnp.exp2((score_ref[block % 2, at] - row_max) * factor)
            part = fold(jnp.add, raised)
            total = part if total is None else total + part
            source, place = divmod(block + at, per)
            o = dot(
                raised.astype(jnp.bfloat16),
                value_refs[source][place * tile : (place + 1) * tile, :],
                ((1,), (0,)),
            )
            summed = o if summed is None else summed + o
        attended = summed / jnp.sum(total, axis=1, keepdims=True)
        here = slice(block * tile, (block + 1) * tile)
        pre = dot(query_ref[here, :], gate_up, ((1,), (0,)))
        gate_pre, up_pre = pre[:, :width], pre[:, width:]
        hidden = (gate_pre * sigmoid(gate_pre) * up_pre).astype(jnp.bfloat16)
        applied = dot(hidden, down, ((1,), (1,)))
        normed = (
            applied
            * lax.rsqrt(jnp.mean(applied * applied, axis=1, keepdims=True) + rms_epsilon)
            * gain
        )
        out_ref[here, :] = (normed + attended).astype(jnp.bfloat16)


def mix(group, bias, queries, keys, values, own_keys, own_values, weights, gain, earlier):
    group_count, rows, features = queries.shape
    heads = features // HD
    width = weights.shape[-1]
    tile = min(256, rows)
    own = pl.BlockSpec((None, rows, HD), lambda h: (group, 0, h))
    passed = pl.BlockSpec((rows, HD), lambda h: (0, h))
    operands = [bias, queries, *keys, own_keys, *values, own_values, weights, gain]
    in_specs = [
        pl.BlockSpec(memory_space=pltpu.SMEM),
        own,
        passed,
        passed,
        own,
        passed,
        passed,
        own,
        pl.BlockSpec((None, 3, HD, width), lambda h: (h, 0, 0, 0)),
        pl.BlockSpec((1, HD), lambda h: (0, h)),
    ]
    aliases = {}
    if earlier is not None:
        aliases = {len(operands): 0}
        operands.append(earlier)
        in_specs.append(pl.BlockSpec(memory_space=pl.ANY))
    return pl.pallas_call(
        functools.partial(mix_kernel, tile, group == 0),
        grid=(heads,),
        in_specs=in_specs,
        out_specs=own,
        out_shape=jax.ShapeDtypeStruct(queries.shape, jnp.bfloat16),
        scratch_shapes=[pltpu.VMEM((2, 2 * rows // tile + 1, tile, tile), jnp.float32)],
        input_output_aliases=aliases,
        cost_estimate=pl.CostEstimate(
            flops=heads * rows * (2 * rows + tile) * HD * 4 * 2,
            bytes_accessed=8 * rows * features * 2,
            transcendentals=heads * rows * (2 * rows + tile),
        ),
        name="attend_and_mix",
    )(*operands)


def layer_kernel(
    moved,
    query_hbm,
    key_hbm,
    value_hbm,
    rate_hbm,
    gate_hbm,
    up_hbm,
    down_hbm,
    step_ref,
    gain_ref,
    mixed_ref,
    final_ref,
    query_buf,
    key_buf,
    value_buf,
    rate_buf,
    first_buf,
    low_buf,
    own_grad,
    own_got,
    far_grad,
    far_got,
    sum_buf,
    cross_buf,
    total_buf,
    score_ref,
    visit_buf,
    part_send_buf,
    part_buf,
    log_send_buf,
    log_buf,
    kept_part,
    kept_norm,
    kept_log,
    local_sem,
    small_sem,
    far_send,
    far_recv,
    near_send,
    near_recv,
    rate_send,
    rate_recv,
    own_send,
    own_recv,
    swap_send,
    swap_recv,
    cross_send,
    cross_recv,
    pass_send,
    pass_recv,
    visit_send,
    visit_recv,
    part_send,
    part_recv,
):
    groups, heads, rows, _ = query_buf.shape
    kept = heads - moved
    rank = lax.axis_index("seq")
    partner = rank + 1 - 2 * (rank % 2)
    across = (rank + 2) % 4
    core = rank % 2
    odd = core == 1
    even = core == 0
    early = rank < 2
    late = rank >= 2
    OWN, FAR, NEAR = 0, groups, 2 * groups
    mesh_ids = pl.DeviceIdType.MESH
    slab = HD // 2

    def lanes(head):
        return pl.ds(pl.multiple_of(head * HD, HD), HD)

    def remote(src, dst, send, recv, to):
        return pltpu.make_async_remote_copy(
            src_ref=src,
            dst_ref=dst,
            send_sem=send,
            recv_sem=recv,
            device_id={"seq": to},
            device_id_type=mesh_ids,
        )

    def far_copy(group, head, which):
        source, target = ((key_hbm, key_buf), (value_hbm, value_buf))[which]
        return remote(
            source.at[group, :, lanes(head)],
            target.at[FAR + group, head],
            far_send.at[group, head, which],
            far_recv.at[group, head, which],
            across,
        )

    def near_copy(group, slot, head, which):
        source, target = ((key_hbm, key_buf), (value_hbm, value_buf))[which]
        return remote(
            source.at[group, :, lanes(head)],
            target.at[NEAR + slot, head],
            near_send.at[slot, head, which],
            near_recv.at[slot, head, which],
            partner,
        )

    def relay_copy(group, slot, head, which):
        target = (key_buf, value_buf)[which]
        return remote(
            target.at[FAR + group, head],
            target.at[NEAR + slot, head],
            near_send.at[slot, head, which],
            near_recv.at[slot, head, which],
            partner,
        )

    def rate_copy():
        return remote(rate_hbm, rate_buf.at[1], rate_send, rate_recv, across)

    def local_copy(group, head, which):
        source = (query_hbm, key_hbm, value_hbm)[which]
        if which == 0:
            target = query_buf.at[group, head]
        else:
            target = (key_buf, value_buf)[which - 1].at[OWN + group, head]
        return pltpu.make_async_copy(
            source.at[group, :, lanes(head)], target, local_sem.at[group, head, which]
        )

    def first_copy(which):
        source = (gate_hbm, up_hbm, down_hbm)[which]
        return pltpu.make_async_copy(source, first_buf.at[:, which], small_sem.at[which])

    def own_rate_copy():
        return pltpu.make_async_copy(rate_hbm, rate_buf.at[0], small_sem.at[3])

    def own_copy(group, head):
        return remote(
            own_grad.at[group, head],
            own_got.at[group, head],
            own_send.at[group, head],
            own_recv.at[group, head],
            partner,
        )

    def swap_copy(group, head):
        return remote(
            far_grad.at[group, head],
            far_got.at[group, head],
            swap_send.at[group, head],
            swap_recv.at[group, head],
            partner,
        )

    def cross_copy(head):
        part = pl.ds(pl.multiple_of(core * slab, slab), slab)
        return remote(
            sum_buf.at[head, :, part],
            cross_buf.at[head, :, part],
            cross_send.at[head],
            cross_recv.at[head],
            across,
        )

    def pass_copy(head):
        part = pl.ds(pl.multiple_of(core * slab, slab), slab)
        return remote(
            cross_buf.at[head, :, part],
            cross_buf.at[head, :, part],
            pass_send.at[head],
            pass_recv.at[head],
            partner,
        )

    def visit_copy(at):
        return remote(
            query_hbm.at[1, :, lanes(kept + at)],
            visit_buf.at[at],
            visit_send.at[at],
            visit_recv.at[at],
            across,
        )

    def part_copy(at):
        return remote(
            part_send_buf.at[at], part_buf.at[at], part_send.at[at, 0], part_recv.at[at, 0], across
        )

    def log_copy(at):
        return remote(
            log_send_buf.at[at], log_buf.at[at], part_send.at[at, 1], part_recv.at[at, 1], across
        )

    def both(make):
        for which in range(2):
            make(which)

    barrier = pltpu.get_barrier_semaphore()
    for peer in (partner, across):
        pl.semaphore_signal(barrier, inc=1, device_id={"seq": peer}, device_id_type=mesh_ids)
    pl.semaphore_wait(barrier, 2)

    rate_copy().start()
    for head in range(heads):
        both(lambda which: far_copy(0, head, which).start())
    own_rate_copy().start()
    for which in range(3):
        first_copy(which).start()
    for group in range(groups):
        for head in range(heads):
            for which in (1, 2, 0):
                local_copy(group, head, which).start()

    @pl.when(early)
    def _():
        for head in range(kept):
            both(lambda which: far_copy(1, head, which).start())

        @pl.when(odd)
        def _():
            for head in range(kept, heads):
                both(lambda which: near_copy(1, 0, head, which).start())

    @pl.when(late)
    def _():
        for at in range(moved):
            visit_copy(at).start()

    @pl.when(even)
    def _():
        for group in range(groups):
            for head in range(heads):
                both(lambda which: near_copy(group, group, head, which).start())

    own_rate_copy().wait()
    for which in range(3):
        first_copy(which).wait()
    low_buf[0] = first_buf[...].astype(jnp.bfloat16)
    for which in range(3):
        final_ref[which] = first_buf[:, which]

    def own_gradients(group, head):
        gradients_of(
            key_buf.at[OWN + group, head],
            value_buf.at[OWN + group, head],
            rate_buf.at[0, group],
            head,
            low_buf.at[group, head],
            own_grad.at[group, head],
        )

    def own_step(head, _):
        local_copy(0, head, 1).wait()
        local_copy(0, head, 2).wait()
        own_gradients(0, head)
        own_copy(0, head).start()
        return 0

    lax.fori_loop(0, heads, own_step, 0)
    rate_copy().wait_recv()

    def sources_of(which, slots, head):
        buf = (key_buf, value_buf)[which]
        return tuple(buf.at[slot, head] for slot in slots)

    def mix_head(group, head, far_slot, near_slot, bias, sources):
        local_copy(group, head, 0).wait()

        @pl.when(jnp.logical_or(group == 1, rank > 0))
        def _():
            both(lambda which: near_copy(group, group, head, which).wait_recv())

        slots = (far_slot, near_slot, OWN + group)
        attend_and_mix(
            bias,
            query_buf.at[group, head],
            sources_of(0, slots, head),
            sources_of(1, slots, head),
            low_buf.at[group, head],
            gain_ref[:, lanes(head)],
            mixed_ref.at[group, :, lanes(head)],
            score_ref,
            sources,
        )

    def group_step(group, _):
        lonely = jnp.logical_and(group == 0, rank == 0)
        far_slot = FAR + jnp.where(late, group, 0)
        near_slot = jnp.where(lonely, OWN, NEAR + group)
        bias = (0.0, jnp.where(lonely, BARRED, 0.0).astype(jnp.float32))

        @pl.when(group == 1)
        def _():
            def sum_step(head, _):
                own_copy(1, head).wait_recv()
                sum_buf[head] = own_grad[1, head] + own_got[1, head]
                return 0

            lax.fori_loop(0, heads, sum_step, 0)

            @pl.when(late)
            def _():
                for head in range(heads):
                    cross_copy(head).start()

            @pl.when(early)
            def _():
                for head in range(kept, heads):
                    cross_copy(head).start()

            def moved_step(at, _):
                head = kept + at

                @pl.when(early)
                def _():
                    visit_copy(at).wait_recv()

                    @pl.when(even)
                    def _():
                        both(lambda which: near_copy(1, 0, head, which).wait_recv())

                    inner_slot = jnp.where(even, NEAR, OWN + 1)
                    barred = (0.0, jnp.where(odd, BARRED, 0.0).astype(jnp.float32))
                    slots = (OWN + 1, inner_slot)
                    attend_part(
                        barred,
                        visit_buf.at[at],
                        sources_of(0, slots, head),
                        sources_of(1, slots, head),
                        part_send_buf.at[at],
                        log_send_buf.at[at],
                        score_ref,
                    )
                    log_copy(at).start()
                    part_copy(at).start()

                @pl.when(late)
                def _():
                    local_copy(1, head, 0).wait()

                    @pl.when(odd)
                    def _():
                        both(lambda which: near_copy(1, 1, head, which).wait_recv())

                    inner_slot = jnp.where(odd, NEAR + 1, OWN + 1)
                    barred = (0.0, jnp.where(even, BARRED, 0.0).astype(jnp.float32))
                    slots = (OWN + 1, inner_slot, OWN + 1)
                    attend_kept(
                        barred,
                        query_buf.at[1, head],
                        sources_of(0, slots, head),
                        sources_of(1, slots, head),
                        low_buf.at[1, head],
                        gain_ref[:, lanes(head)],
                        kept_part.at[at],
                        kept_norm.at[at],
                        kept_log.at[at],
                        score_ref,
                    )

                return 0

            lax.fori_loop(0, moved, moved_step, 0)

        def shares(head):
            return jnp.logical_or(group == 0, jnp.logical_and(late, head < kept))

        def head_step(head, _):
            shared = shares(head)
            low = low_buf.at[group, head]

            @pl.when(group == 0)
            def _():
                own_copy(0, head).wait_recv()
                sum_buf[head] = own_grad[0, head] + own_got[0, head]

            @pl.when(shared)
            def _():
                both(lambda which: far_copy(group, head, which).wait_recv())

                @pl.when(odd)
                def _():
                    slot = jnp.where(late, group, 1)
                    both(lambda which: relay_copy(group, slot, head, which).start())

                gradients_of(
                    key_buf.at[FAR + group, head],
                    value_buf.at[FAR + group, head],
                    rate_buf.at[1, group],
                    head,
                    low,
                    far_grad.at[group, head],
                )
                swap_copy(group, head).start()

            @pl.when(jnp.logical_not(shared))
            def _():
                cross_copy(head).wait_recv()
                pass_copy(head).start()

            remains = jnp.where(early, head >= heads - 2, head < kept)

            @pl.when(jnp.logical_and(early, group == 0))
            def _():
                mix_head(0, head, FAR, near_slot, bias, (1, 2))

            @pl.when(jnp.logical_and(jnp.logical_or(late, group == 1), jnp.logical_or(group == 0, remains)))
            def _():
                mix_head(group, head, far_slot, near_slot, (0.0, 0.0), (0, 1, 2))

            return 0

        def pair_step(pair, _):
            lax.fori_loop(2 * pair, 2 * pair + 2, head_step, 0)
            for at in range(2):
                head = 2 * pair + at

                @pl.when(shares(head))
                def _():
                    swap_copy(group, head).wait_recv()
                    total_buf[at] = sum_buf[head] + (far_grad[group, head] + far_got[group, head])

                @pl.when(jnp.logical_not(shares(head)))
                def _():
                    pass_copy(head).wait_recv()
                    total_buf[at] = sum_buf[head] + cross_buf[head]

            renew_pair(
                total_buf,
                first_buf.at[pl.ds(2 * pair, 2)],
                final_ref.at[:, pl.ds(2 * pair, 2)],
                [step_ref[2 * pair + at] for at in range(2)],
            )

            def after_step(head, _):
                low_buf[1, head] = final_ref[:, head].astype(jnp.bfloat16)
                local_copy(1, head, 1).wait()
                local_copy(1, head, 2).wait()
                own_gradients(1, head)
                own_copy(1, head).start()

                @pl.when(jnp.logical_and(early, head < heads - 2))
                def _():
                    mix_head(1, head, FAR, NEAR + 1, (0.0, 0.0), (0, 1, 2))

                return 0

            @pl.when(group == 0)
            def _():
                lax.fori_loop(2 * pair, 2 * pair + 2, after_step, 0)

            return 0

        lax.fori_loop(0, heads // 2, pair_step, 0)
        return 0

    lax.fori_loop(0, groups, group_step, 0)

    @pl.when(late)
    def _():
        def merge_step(at, _):
            log_copy(at).wait_recv()
            part_copy(at).wait_recv()
            merge_parts(
                kept_part.at[at],
                kept_norm.at[at],
                kept_log.at[at],
                part_buf.at[at],
                log_buf.at[at],
                mixed_ref.at[1, :, lanes(kept + at)],
            )
            return 0

        lax.fori_loop(0, moved, merge_step, 0)

    rate_copy().wait_send()
    for head in range(heads):
        both(lambda which: far_copy(0, head, which).wait_send())
        for group in range(groups):
            own_copy(group, head).wait_send()
        swap_copy(0, head).wait_send()

    @pl.when(early)
    def _():
        for head in range(kept):
            both(lambda which: far_copy(1, head, which).wait_send())
        for head in range(kept, heads):
            cross_copy(head).wait_send()
        for head in range(heads):
            pass_copy(head).wait_send()
        for at in range(moved):
            log_copy(at).wait_send()
            part_copy(at).wait_send()

        @pl.when(odd)
        def _():
            for head in range(kept, heads):
                both(lambda which: near_copy(1, 0, head, which).wait_send())

    @pl.when(even)
    def _():
        for group in range(groups):
            for head in range(heads):
                both(lambda which: near_copy(group, group, head, which).wait_send())

    @pl.when(odd)
    def _():
        for head in range(heads):
            both(lambda which: relay_copy(0, jnp.where(late, 0, 1), head, which).wait_send())

    @pl.when(late)
    def _():
        for at in range(moved):
            visit_copy(at).wait_send()
        for head in range(heads):
            cross_copy(head).wait_send()
        for head in range(kept, heads):
            pass_copy(head).wait_send()
        for head in range(kept):
            swap_copy(1, head).wait_send()

        @pl.when(odd)
        def _():
            for head in range(kept):
                both(lambda which: relay_copy(1, 1, head, which).wait_send())


def gradients_of(key_ref, value_ref, rate_ref, head, low, out_ref):
    rows = key_ref.shape[0]
    width = low.shape[-1]
    chunk = min(256, rows)
    gate_up = jnp.concatenate([low[0], low[1]], axis=1)
    down = low[2]
    totals = None
    for start in range(0, rows, chunk):
        part = pl.ds(start, chunk)
        keys = key_ref[part, :]
        columns = []
        for at in range(start, start + chunk, HD):
            rates = rate_ref[:, pl.ds(at, HD)]
            place = lax.broadcasted_iota(jnp.int32, rates.shape, 0)
            row = jnp.sum(jnp.where(place == head, rates, 0.0), axis=0, keepdims=True)
            columns.append(jnp.transpose(jnp.broadcast_to(row, (HD, HD))))
        rate = jnp.concatenate(columns, axis=0)
        out_grad = (-rate * value_ref[part, :].astype(jnp.float32)).astype(jnp.bfloat16)
        pre = dot(keys, gate_up, ((1,), (0,)))
        gate_pre, up_pre = pre[:, :width], pre[:, width:]
        squash = sigmoid(gate_pre)
        active = gate_pre * squash
        hidden = (active * up_pre).astype(jnp.bfloat16)
        hidden_grad = dot(out_grad, down, ((1,), (0,)))
        up_grad = (hidden_grad * active).astype(jnp.bfloat16)
        gate_grad = (hidden_grad * up_pre * squash * (1.0 + gate_pre * (1.0 - squash))).astype(
            jnp.bfloat16
        )
        terms = (
            dot(keys, gate_grad, ((0,), (0,))),
            dot(keys, up_grad, ((0,), (0,))),
            dot(out_grad, hidden, ((0,), (0,))),
        )
        for which in range(3):
            if start == 0:
                out_ref[which] = terms[which]
            else:
                out_ref[which] += terms[which]


def renew_pair(gradient_ref, first_ref, current_ref, steps):
    slots = [(at, which) for at in range(2) for which in range(3)]
    matrices = []
    for at, which in slots:
        gradient = gradient_ref[at, which]
        frobenius = jnp.sqrt(jnp.sum(gradient * gradient, keepdims=True))
        matrices.append(gradient / (frobenius + frob_epsilon))
    matrices = sweep_all(matrices)
    for (at, which), matrix in zip(slots, matrices):
        first = first_ref[at, which]
        target = jnp.sqrt(jnp.sum(first * first, axis=0, keepdims=True))
        stepped = current_ref[which, at] - steps[at] * matrix
        length = jnp.sqrt(jnp.sum(stepped * stepped, axis=0, keepdims=True))
        current_ref[which, at] = stepped * (target / (length + column_epsilon))


def sweep_all(matrices):
    for sweep in range(NS_STEPS):
        pairs = [split(matrix) for matrix in matrices]
        grams = [
            dot(
                jnp.concatenate([high, high, rest], axis=1),
                jnp.concatenate([high, rest, high], axis=1),
                ((1,), (1,)),
            )
            for high, rest in pairs
        ]
        polynomials = []
        for gram in grams:
            high, rest = split(gram)
            squared = dot(
                jnp.concatenate([high, high, rest], axis=1),
                jnp.concatenate([high, rest, high], axis=0),
                ((1,), (0,)),
            )
            polynomials.append(coeff_second * gram + coeff_third * squared)
        moved = []
        for polynomial, (high, rest), matrix in zip(polynomials, pairs, matrices):
            poly_high, poly_rest = split(polynomial)
            moved.append(
                coeff_first * matrix
                + dot(
                    jnp.concatenate([poly_high, poly_high, poly_rest], axis=1),
                    jnp.concatenate([high, rest, high], axis=0),
                    ((1,), (0,)),
                )
            )
        matrices = moved
    return matrices


def attend(bias, query_ref, key_refs, value_refs, score_ref, sources, emit):
    rows = query_ref.shape[0]
    tile = min(256, rows)
    per = rows // tile
    span = 2 * per + 1
    factor = math.log2(math.e) / math.sqrt(HD)
    row = lax.broadcasted_iota(jnp.int32, (tile, tile), 0)
    column = lax.broadcasted_iota(jnp.int32, (tile, tile), 1)
    later = column > row

    def fold(op, a):
        folded = a[:, :HD]
        for at in range(HD, tile, HD):
            folded = op(folded, a[:, at : at + HD])
        return folded

    def tiles(block):
        return [at for at in range(span) if (block + at) // per in sources]

    def score(block, at, peak):
        source, place = divmod(block + at, per)
        queries = query_ref[block * tile : (block + 1) * tile, :]
        s = dot(queries, key_refs[source][place * tile : (place + 1) * tile, :], ((1,), (1,)))
        if at == 0:
            s = jnp.where(later, s, EXCLUDED)
        if at == span - 1:
            s = jnp.where(later, EXCLUDED, s)
        score_ref[block % 2, at] = s
        top = fold(jnp.maximum, s)
        if source < 2:
            top = top + bias[source]
        return top if peak is None else jnp.maximum(peak, top)

    peak = None
    for at in tiles(0):
        peak = score(0, at, peak)
    for block in range(per):
        row_max = jnp.max(peak, axis=1, keepdims=True)
        base = (row_max - bias[0], row_max - bias[1], row_max)
        ahead = tiles(block + 1) if block + 1 < per else []
        peak = None
        total = None
        summed = None
        for at in tiles(block):
            if ahead:
                peak = score(block + 1, ahead.pop(0), peak)
            source, place = divmod(block + at, per)
            raised = jnp.exp2((score_ref[block % 2, at] - base[source]) * factor)
            part = fold(jnp.add, raised)
            total = part if total is None else total + part
            o = dot(
                raised.astype(jnp.bfloat16),
                value_refs[source][place * tile : (place + 1) * tile, :],
                ((1,), (0,)),
            )
            summed = o if summed is None else summed + o
        for at in ahead:
            peak = score(block + 1, at, peak)
        weight = jnp.sum(total, axis=1, keepdims=True)
        here = slice(block * tile, (block + 1) * tile)
        emit(here, summed / weight, row_max * factor, weight)


def apply_weights(queries, low, gain):
    width = low.shape[-1]
    gate_up = jnp.concatenate([low[0], low[1]], axis=1)
    pre = dot(queries, gate_up, ((1,), (0,)))
    gate_pre, up_pre = pre[:, :width], pre[:, width:]
    hidden = (gate_pre * sigmoid(gate_pre) * up_pre).astype(jnp.bfloat16)
    applied = dot(hidden, low[2], ((1,), (1,)))
    return (
        applied
        * lax.rsqrt(jnp.mean(applied * applied, axis=1, keepdims=True) + rms_epsilon)
        * gain
    )


def attend_and_mix(
    bias, query_ref, key_refs, value_refs, low, gain, out_ref, score_ref, sources
):
    def emit(here, attended, top, weight):
        normed = apply_weights(query_ref[here, :], low, gain)
        out_ref[here, :] = (normed + attended).astype(jnp.bfloat16)

    attend(bias, query_ref, key_refs, value_refs, score_ref, sources, emit)


def log_sum(top, weight):
    return top + math.log2(math.e) * jnp.log(weight)


def attend_part(bias, query_ref, key_refs, value_refs, part_ref, log_ref, score_ref):
    def emit(here, attended, top, weight):
        part_ref[here, :] = attended.astype(jnp.bfloat16)
        logs = jnp.broadcast_to(log_sum(top, weight), attended.shape)
        for at in range(0, attended.shape[0], HD):
            place = (here.start + at) // HD
            log_ref[place : place + 1, :] = jnp.transpose(logs[at : at + HD])[:1]

    attend(bias, query_ref, key_refs, value_refs, score_ref, (0, 1), emit)


def attend_kept(
    bias, query_ref, key_refs, value_refs, low, gain, part_ref, norm_ref, log_ref, score_ref
):
    def emit(here, attended, top, weight):
        norm_ref[here, :] = apply_weights(query_ref[here, :], low, gain)
        part_ref[here, :] = attended
        log_ref[here, :] = jnp.broadcast_to(log_sum(top, weight), attended.shape)

    attend(bias, query_ref, key_refs, value_refs, score_ref, (1, 2), emit)


def merge_parts(part_ref, norm_ref, log_ref, other_ref, other_log_ref, out_ref):
    for start in range(0, part_ref.shape[0], HD):
        here = slice(start, start + HD)
        place = start // HD
        mine = log_ref[here, :]
        other = jnp.transpose(jnp.broadcast_to(other_log_ref[place : place + 1, :], (HD, HD)))
        top = jnp.maximum(mine, other)
        mine, other = jnp.exp2(mine - top), jnp.exp2(other - top)
        attended = (mine * part_ref[here, :] + other * other_ref[here, :].astype(jnp.float32)) / (
            mine + other
        )
        out_ref[here, :] = (norm_ref[here, :] + attended).astype(jnp.bfloat16)


def whole_layer(queries, keys, values, rates, gate, up, down, steps, gain):
    groups, rows, features = queries.shape
    heads = features // HD
    moved = heads // 2
    width = gate.shape[-1]
    tile = min(256, rows)
    span = 2 * (rows // tile) + 1
    dma = pltpu.SemaphoreType.DMA
    brief, full = jnp.bfloat16, jnp.float32
    matrices = (3, HD, width)
    return pl.pallas_call(
        functools.partial(layer_kernel, moved),
        in_specs=[pl.BlockSpec(memory_space=pltpu.HBM)] * 7
        + [pl.BlockSpec(memory_space=pltpu.SMEM), pl.BlockSpec(memory_space=pltpu.VMEM)],
        out_specs=[pl.BlockSpec(memory_space=pltpu.VMEM)] * 2,
        out_shape=[
            pltpu.VMEM(queries.shape, brief),
            pltpu.VMEM((3, heads, HD, width), full),
        ],
        scratch_shapes=[
            pltpu.VMEM((groups, heads, rows, HD), brief),
            pltpu.VMEM((3 * groups, heads, rows, HD), brief),
            pltpu.VMEM((3 * groups, heads, rows, HD), brief),
            pltpu.VMEM((2, groups, heads, rows), full),
            pltpu.VMEM((heads,) + matrices, full),
            pltpu.VMEM((groups, heads) + matrices, brief),
            pltpu.VMEM((groups, heads) + matrices, full),
            pltpu.VMEM((groups, heads) + matrices, full),
            pltpu.VMEM((groups, heads) + matrices, full),
            pltpu.VMEM((groups, heads) + matrices, full),
            pltpu.VMEM((heads,) + matrices, full),
            pltpu.VMEM((heads,) + matrices, full),
            pltpu.VMEM((2,) + matrices, full),
            pltpu.VMEM((2, span, tile, tile), full),
            pltpu.VMEM((moved, rows, HD), brief),
            pltpu.VMEM((moved, rows, HD), brief),
            pltpu.VMEM((moved, rows, HD), brief),
            pltpu.VMEM((moved, rows // HD, HD), full),
            pltpu.VMEM((moved, rows // HD, HD), full),
            pltpu.VMEM((moved, rows, HD), full),
            pltpu.VMEM((moved, rows, HD), full),
            pltpu.VMEM((moved, rows, HD), full),
            dma((groups, heads, 3)),
            dma((4,)),
            dma((groups, heads, 2)),
            dma((groups, heads, 2)),
            dma((groups, heads, 2)),
            dma((groups, heads, 2)),
            dma,
            dma,
            dma((groups, heads)),
            dma((groups, heads)),
            dma((groups, heads)),
            dma((groups, heads)),
            dma((heads,)),
            dma((heads,)),
            dma((heads,)),
            dma((heads,)),
            dma((moved,)),
            dma((moved,)),
            dma((moved, 2)),
            dma((moved, 2)),
        ],
        compiler_params=pltpu.CompilerParams(
            collective_id=0, has_side_effects=True, vmem_limit_bytes=VMEM_GRANT
        ),
        name="whole_layer",
    )(queries, keys, values, rates, gate, up, down, steps, gain)


def body(
    query_vectors,
    key_vectors,
    value_vectors,
    token_rates,
    gate_weight,
    up_weight,
    down_weight,
    step_sizes,
    norm_gain,
):
    group_count, tok_rows, feature_width = query_vectors.shape
    head_count = feature_width // HD
    rank = lax.axis_index("seq")
    count = lax.axis_size("seq")
    if count == 4 and group_count == 2 and head_count % 2 == 0:
        return whole_layer(
            query_vectors,
            key_vectors,
            value_vectors,
            token_rates,
            gate_weight,
            up_weight,
            down_weight,
            step_sizes,
            norm_gain[None, :],
        )
    swap = [(i, i ^ 1) for i in range(count)]
    ring = lambda d: [(i, (i + d) % count) for i in range(count)]
    shift = lambda a, route: lax.ppermute(a, "seq", route)
    odd = rank % 2 == 1

    far, near = [], []
    for group in range(group_count):
        far_pair, near_pair = [], []
        for tokens in (key_vectors, value_vectors):
            if group == 0:
                sent = tokens[0]
                route = [(i, i + 2) for i in range(count - 2)]
            else:
                sent = jnp.where(rank >= count - 2, tokens[group - 1], tokens[group])
                route = ring(2)
            far_block = shift(sent, route)
            far_pair.append(far_block)
            near_pair.append(shift(jnp.where(odd, far_block, tokens[group]), swap))
        far.append(far_pair)
        near.append(near_pair)

    spread = head_count == count
    first = jnp.stack([gate_weight, up_weight, down_weight], axis=1)
    rates = jnp.transpose(token_rates, (0, 2, 1))
    gain = norm_gain[None, :]
    bias = jnp.where(rank >= jnp.array([2, 1]), 0.0, EXCLUDED).astype(jnp.float32)
    pair_count = count // 2
    pair, core = rank // 2, rank % 2
    if spread:
        first_mine = lax.dynamic_slice_in_dim(first, rank, 1, 0)
        steps = lax.dynamic_slice_in_dim(step_sizes, rank, 1, 0)
    else:
        first_mine, steps = first, step_sizes
    weights_mine = first_mine
    low = first

    def gather(mine):
        arrived = [mine[0]] + [shift(mine[0], ring(2 * d)) for d in range(1, pair_count)]
        column = jnp.stack(arrived)
        other = shift(column, swap)
        blocks = []
        for head in range(head_count):
            at = (pair - head // 2) % pair_count
            pick = lambda a: lax.dynamic_index_in_dim(a, at, 0, keepdims=False)
            blocks.append(jnp.where(core == head % 2, pick(column), pick(other)))
        return blocks

    mixed = None
    for group in range(group_count):
        gradients = group_gradients(group, key_vectors, value_vectors, rates, low)
        last = group + 1 == group_count
        if spread:
            by_core = gradients.reshape((pair_count, 2) + gradients.shape[1:])
            kept = lax.dynamic_index_in_dim(by_core, core, 1, keepdims=False)
            given = lax.dynamic_index_in_dim(by_core, 1 - core, 1, keepdims=False)
            pair_sum = kept + shift(given, swap)
            block = lambda d: lax.dynamic_slice_in_dim(pair_sum, (pair + d) % pair_count, 1, 0)
            parts = [block(0)] + [shift(block(d), ring(2 * d)) for d in range(1, pair_count)]
        else:
            parts = [lax.psum(gradients, "seq")]
        mixed = mix(
            group,
            bias,
            query_vectors,
            (far[group][0], near[group][0]),
            (far[group][1], near[group][1]),
            key_vectors,
            value_vectors,
            low,
            gain,
            mixed,
        )
        weights_mine, low_mine = renew(parts, first_mine, weights_mine, steps)
        if not spread:
            low = low_mine
        elif not last:
            low = jnp.stack(gather(low_mine))
    if spread:
        final = jnp.stack(gather(weights_mine), axis=1)
    else:
        final = jnp.transpose(weights_mine, (1, 0, 2, 3))
    return (mixed, final)


def solution(mesh):
    return jax.shard_map(
        body,
        mesh=mesh,
        in_specs=(
            P("batch", "seq", "head"),
            P("batch", "seq", "head"),
            P("batch", "seq", "head"),
            P("batch", "head", "seq"),
            P("head", None, None),
            P("head", None, None),
            P("head", None, None),
            P("head"),
            P("head"),
        ),
        out_specs=(P("batch", "seq", "head"), P("batch", "head", None, None)),
        check_vma=False,
    )
```

```python
import functools
import math

import jax
import jax.numpy as jnp
from jax import lax
from jax.experimental import pallas as pl
from jax.experimental.pallas import tpu as pltpu
from jax.sharding import PartitionSpec as P

HD = 128
NS_STEPS = 5

coeff_first = 3.4445
coeff_second = -4.775
coeff_third = 2.0315
frob_epsilon = 1e-07
rms_epsilon = 1e-06
column_epsilon = 1e-06
EXCLUDED = -1e30
BARRED = -3e30
VMEM_GRANT = 51 * 2**20


def dot(a, b, dims):
    return lax.dot_general(a, b, (dims, ((), ())), preferred_element_type=jnp.float32)


def sigmoid(a):
    return 0.5 * jnp.tanh(0.5 * a) + 0.5


def grads_kernel(chunk, key_ref, value_ref, rate_ref, weight_ref, out_ref):
    head = pl.program_id(0)
    width = weight_ref.shape[-1]
    rows = key_ref.shape[0]
    gate_up = jnp.concatenate([weight_ref[0], weight_ref[1]], axis=1).astype(jnp.bfloat16)
    down = weight_ref[2].astype(jnp.bfloat16)
    for start in range(0, rows, chunk):
        part = pl.ds(start, chunk)
        keys = key_ref[part, :]
        rates = rate_ref[part, :]
        lane = lax.broadcasted_iota(jnp.int32, rates.shape, 1)
        rate = jnp.sum(jnp.where(lane == head, rates, 0.0), axis=1, keepdims=True)
        out_grad = (-rate * value_ref[part, :].astype(jnp.float32)).astype(jnp.bfloat16)
        pre = dot(keys, gate_up, ((1,), (0,)))
        gate_pre, up_pre = pre[:, :width], pre[:, width:]
        squash = sigmoid(gate_pre)
        active = gate_pre * squash
        hidden = (active * up_pre).astype(jnp.bfloat16)
        hidden_grad = dot(out_grad, down, ((1,), (0,)))
        up_grad = (hidden_grad * active).astype(jnp.bfloat16)
        gate_grad = (hidden_grad * up_pre * squash * (1.0 + gate_pre * (1.0 - squash))).astype(
            jnp.bfloat16
        )
        terms = (
            dot(keys, gate_grad, ((0,), (0,))),
            dot(keys, up_grad, ((0,), (0,))),
            dot(out_grad, hidden, ((0,), (0,))),
        )
        for which in range(3):
            if start == 0:
                out_ref[which] = terms[which]
            else:
                out_ref[which] += terms[which]


def group_gradients(group, keys, values, rates, weights):
    _, rows, features = keys.shape
    heads = features // HD
    width = weights.shape[-1]
    token_spec = pl.BlockSpec((None, rows, HD), lambda h: (group, 0, h))
    return pl.pallas_call(
        functools.partial(grads_kernel, min(256, rows)),
        grid=(heads,),
        in_specs=[
            token_spec,
            token_spec,
            pl.BlockSpec((None, rows, heads), lambda h: (group, 0, 0)),
            pl.BlockSpec((None, 3, HD, width), lambda h: (h, 0, 0, 0)),
        ],
        out_specs=pl.BlockSpec((None, 3, HD, width), lambda h: (h, 0, 0, 0)),
        out_shape=jax.ShapeDtypeStruct((heads, 3, HD, width), jnp.float32),
        cost_estimate=pl.CostEstimate(
            flops=6 * 2 * 2 * heads * rows * HD * width,
            bytes_accessed=2 * rows * features * 2 + heads * 3 * HD * width * 8,
            transcendentals=heads * rows * width,
        ),
        name="group_gradients",
    )(keys, values, rates, weights)


def split(a):
    high = a.astype(jnp.bfloat16)
    return high, (a - high.astype(jnp.float32)).astype(jnp.bfloat16)


def renew_kernel(parts, *refs):
    grad_refs = refs[:parts]
    first_ref, weight_ref, step_ref, new_ref, low_ref = refs[parts:]
    step = step_ref[pl.program_id(0)]
    matrices = []
    for which in range(3):
        gradient = grad_refs[0][which]
        for ref in grad_refs[1:]:
            gradient = gradient + ref[which]
        frobenius = jnp.sqrt(jnp.sum(gradient * gradient, keepdims=True))
        matrices.append(gradient / (frobenius + frob_epsilon))
    for sweep in range(NS_STEPS):
        pairs = [split(matrix) for matrix in matrices]
        grams = [
            dot(
                jnp.concatenate([high, high, rest], axis=1),
                jnp.concatenate([high, rest, high], axis=1),
                ((1,), (1,)),
            )
            for high, rest in pairs
        ]
        polynomials = []
        for gram in grams:
            high, rest = split(gram)
            squared = dot(
                jnp.concatenate([high, high, rest], axis=1),
                jnp.concatenate([high, rest, high], axis=0),
                ((1,), (0,)),
            )
            polynomials.append(coeff_second * gram + coeff_third * squared)
        moved = []
        for polynomial, (high, rest), matrix in zip(polynomials, pairs, matrices):
            poly_high, poly_rest = split(polynomial)
            moved.append(
                coeff_first * matrix
                + dot(
                    jnp.concatenate([poly_high, poly_high, poly_rest], axis=1),
                    jnp.concatenate([high, rest, high], axis=0),
                    ((1,), (0,)),
                )
            )
        matrices = moved
    for which in range(3):
        first = first_ref[which]
        target = jnp.sqrt(jnp.sum(first * first, axis=0, keepdims=True))
        stepped = weight_ref[which] - step * matrices[which]
        length = jnp.sqrt(jnp.sum(stepped * stepped, axis=0, keepdims=True))
        renewed = stepped * (target / (length + column_epsilon))
        new_ref[which] = renewed
        low_ref[which] = renewed.astype(jnp.bfloat16)


def renew(gradients, first, weights, steps):
    heads, _, _, width = weights.shape
    spec = pl.BlockSpec((None, 3, HD, width), lambda h: (h, 0, 0, 0))
    return pl.pallas_call(
        functools.partial(renew_kernel, len(gradients)),
        grid=(heads,),
        in_specs=[spec] * (len(gradients) + 2) + [pl.BlockSpec(memory_space=pltpu.SMEM)],
        out_specs=[spec, spec],
        out_shape=[
            jax.ShapeDtypeStruct(weights.shape, jnp.float32),
            jax.ShapeDtypeStruct(weights.shape, jnp.bfloat16),
        ],
        cost_estimate=pl.CostEstimate(
            flops=heads * 3 * NS_STEPS * 10 * HD * HD * width * 4,
            bytes_accessed=heads * 3 * HD * width * 20,
            transcendentals=0,
        ),
        name="renew_weights",
    )(*gradients, first, weights, steps)


def mix_kernel(
    tile,
    guarded,
    bias_ref,
    query_ref,
    key_far,
    key_near,
    key_own,
    value_far,
    value_near,
    value_own,
    weight_ref,
    gain_ref,
    *rest,
):
    out_ref, score_ref = rest[-2:]
    rows = query_ref.shape[0]
    width = weight_ref.shape[-1]
    per = rows // tile
    blocks = per
    span = 2 * per + 1
    factor = math.log2(math.e) / math.sqrt(HD)
    key_refs = (key_far, key_near, key_own)
    value_refs = (value_far, value_near, value_own)
    gate_up = jnp.concatenate([weight_ref[0], weight_ref[1]], axis=1).astype(jnp.bfloat16)
    down = weight_ref[2].astype(jnp.bfloat16)
    gain = gain_ref[...]
    row = lax.broadcasted_iota(jnp.int32, (tile, tile), 0)
    column = lax.broadcasted_iota(jnp.int32, (tile, tile), 1)
    later = column > row

    def fold(op, a):
        folded = a[:, :HD]
        for at in range(HD, tile, HD):
            folded = op(folded, a[:, at : at + HD])
        return folded

    def score(block, at, peak):
        source, place = divmod(block + at, per)
        queries = query_ref[block * tile : (block + 1) * tile, :]
        s = dot(queries, key_refs[source][place * tile : (place + 1) * tile, :], ((1,), (1,)))
        if at == 0:
            s = jnp.where(later, s, EXCLUDED)
        if at == span - 1:
            s = jnp.where(later, EXCLUDED, s)
        if guarded and source < 2:
            s = s + bias_ref[source]
        score_ref[block % 2, at] = s
        top = fold(jnp.maximum, s)
        return top if peak is None else jnp.maximum(peak, top)

    peak = None
    for at in range(span):
        peak = score(0, at, peak)
    for block in range(blocks):
        row_max = jnp.max(peak, axis=1, keepdims=True)
        peak = None
        total = None
        summed = None
        for at in range(span):
            if block + 1 < blocks:
                peak = score(block + 1, at, peak)
            raised = jnp.exp2((score_ref[block % 2, at] - row_max) * factor)
            part = fold(jnp.add, raised)
            total = part if total is None else total + part
            source, place = divmod(block + at, per)
            o = dot(
                raised.astype(jnp.bfloat16),
                value_refs[source][place * tile : (place + 1) * tile, :],
                ((1,), (0,)),
            )
            summed = o if summed is None else summed + o
        attended = summed / jnp.sum(total, axis=1, keepdims=True)
        here = slice(block * tile, (block + 1) * tile)
        pre = dot(query_ref[here, :], gate_up, ((1,), (0,)))
        gate_pre, up_pre = pre[:, :width], pre[:, width:]
        hidden = (gate_pre * sigmoid(gate_pre) * up_pre).astype(jnp.bfloat16)
        applied = dot(hidden, down, ((1,), (1,)))
        normed = (
            applied
            * lax.rsqrt(jnp.mean(applied * applied, axis=1, keepdims=True) + rms_epsilon)
            * gain
        )
        out_ref[here, :] = (normed + attended).astype(jnp.bfloat16)


def mix(group, bias, queries, keys, values, own_keys, own_values, weights, gain, earlier):
    group_count, rows, features = queries.shape
    heads = features // HD
    width = weights.shape[-1]
    tile = min(256, rows)
    own = pl.BlockSpec((None, rows, HD), lambda h: (group, 0, h))
    passed = pl.BlockSpec((rows, HD), lambda h: (0, h))
    operands = [bias, queries, *keys, own_keys, *values, own_values, weights, gain]
    in_specs = [
        pl.BlockSpec(memory_space=pltpu.SMEM),
        own,
        passed,
        passed,
        own,
        passed,
        passed,
        own,
        pl.BlockSpec((None, 3, HD, width), lambda h: (h, 0, 0, 0)),
        pl.BlockSpec((1, HD), lambda h: (0, h)),
    ]
    aliases = {}
    if earlier is not None:
        aliases = {len(operands): 0}
        operands.append(earlier)
        in_specs.append(pl.BlockSpec(memory_space=pl.ANY))
    return pl.pallas_call(
        functools.partial(mix_kernel, tile, group == 0),
        grid=(heads,),
        in_specs=in_specs,
        out_specs=own,
        out_shape=jax.ShapeDtypeStruct(queries.shape, jnp.bfloat16),
        scratch_shapes=[pltpu.VMEM((2, 2 * rows // tile + 1, tile, tile), jnp.float32)],
        input_output_aliases=aliases,
        cost_estimate=pl.CostEstimate(
            flops=heads * rows * (2 * rows + tile) * HD * 4 * 2,
            bytes_accessed=8 * rows * features * 2,
            transcendentals=heads * rows * (2 * rows + tile),
        ),
        name="attend_and_mix",
    )(*operands)


def layer_kernel(
    moved,
    query_hbm,
    key_hbm,
    value_hbm,
    rate_hbm,
    gate_hbm,
    up_hbm,
    down_hbm,
    step_ref,
    gain_ref,
    mixed_ref,
    final_ref,
    part_buf,
    log_buf,
    kept_part,
    kept_norm,
    kept_log,
    query_buf,
    key_buf,
    value_buf,
    rate_buf,
    first_buf,
    low_buf,
    own_grad,
    own_got,
    far_grad,
    far_got,
    sum_buf,
    cross_buf,
    total_buf,
    score_ref,
    visit_buf,
    part_send_buf,
    log_send_buf,
    local_sem,
    small_sem,
    far_send,
    far_recv,
    near_send,
    near_recv,
    rate_send,
    rate_recv,
    own_send,
    own_recv,
    swap_send,
    swap_recv,
    cross_send,
    cross_recv,
    pass_send,
    pass_recv,
    visit_send,
    visit_recv,
    part_send,
    part_recv,
):
    groups, heads, rows, _ = query_buf.shape
    rank = lax.axis_index("seq")
    partner = rank + 1 - 2 * (rank % 2)
    across = (rank + 2) % 4
    core = rank % 2
    odd = core == 1
    even = core == 0
    early = rank < 2
    late = rank >= 2
    OWN, FAR, NEAR = 0, groups, 2 * groups
    mesh_ids = pl.DeviceIdType.MESH
    slab = HD // 2

    def lanes(head):
        return pl.ds(pl.multiple_of(head * HD, HD), HD)

    def remote(src, dst, send, recv, to):
        return pltpu.make_async_remote_copy(
            src_ref=src,
            dst_ref=dst,
            send_sem=send,
            recv_sem=recv,
            device_id={"seq": to},
            device_id_type=mesh_ids,
        )

    def far_copy(group, head, which):
        source, target = ((key_hbm, key_buf), (value_hbm, value_buf))[which]
        return remote(
            source.at[group, :, lanes(head)],
            target.at[FAR + group, head],
            far_send.at[group, head, which],
            far_recv.at[group, head, which],
            across,
        )

    def near_copy(group, slot, head, which):
        source, target = ((key_hbm, key_buf), (value_hbm, value_buf))[which]
        return remote(
            source.at[group, :, lanes(head)],
            target.at[NEAR + slot, head],
            near_send.at[slot, head, which],
            near_recv.at[slot, head, which],
            partner,
        )

    def relay_copy(group, slot, head, which):
        target = (key_buf, value_buf)[which]
        return remote(
            target.at[FAR + group, head],
            target.at[NEAR + slot, head],
            near_send.at[slot, head, which],
            near_recv.at[slot, head, which],
            partner,
        )

    def rate_copy():
        return remote(rate_hbm, rate_buf.at[1], rate_send, rate_recv, across)

    def local_copy(group, head, which):
        source = (query_hbm, key_hbm, value_hbm)[which]
        if which == 0:
            target = query_buf.at[group, head]
        else:
            target = (key_buf, value_buf)[which - 1].at[OWN + group, head]
        return pltpu.make_async_copy(
            source.at[group, :, lanes(head)], target, local_sem.at[group, head, which]
        )

    def first_copy(which):
        source = (gate_hbm, up_hbm, down_hbm)[which]
        return pltpu.make_async_copy(source, first_buf.at[:, which], small_sem.at[which])

    def own_rate_copy():
        return pltpu.make_async_copy(rate_hbm, rate_buf.at[0], small_sem.at[3])

    def own_copy(group, head):
        return remote(
            own_grad.at[group, head],
            own_got.at[group, head],
            own_send.at[group, head],
            own_recv.at[group, head],
            partner,
        )

    def swap_copy(group, head):
        return remote(
            far_grad.at[group, head],
            far_got.at[group, head],
            swap_send.at[group, head],
            swap_recv.at[group, head],
            partner,
        )

    def cross_copy(head):
        part = pl.ds(pl.multiple_of(core * slab, slab), slab)
        return remote(
            sum_buf.at[head, :, part],
            cross_buf.at[head, :, part],
            cross_send.at[head],
            cross_recv.at[head],
            across,
        )

    def pass_copy(head):
        part = pl.ds(pl.multiple_of(core * slab, slab), slab)
        return remote(
            cross_buf.at[head, :, part],
            cross_buf.at[head, :, part],
            pass_send.at[head],
            pass_recv.at[head],
            partner,
        )

    def visit_copy(at):
        return remote(
            query_hbm.at[1, :, lanes(at)],
            visit_buf.at[at],
            visit_send.at[at],
            visit_recv.at[at],
            across,
        )

    def part_copy(at):
        return remote(
            part_send_buf.at[at], part_buf.at[at], part_send.at[at, 0], part_recv.at[at, 0], across
        )

    def log_copy(at):
        return remote(
            log_send_buf.at[at], log_buf.at[at], part_send.at[at, 1], part_recv.at[at, 1], across
        )

    def both(make):
        for which in range(2):
            make(which)

    barrier = pltpu.get_barrier_semaphore()
    for peer in (partner, across):
        pl.semaphore_signal(barrier, inc=1, device_id={"seq": peer}, device_id_type=mesh_ids)
    pl.semaphore_wait(barrier, 2)

    rate_copy().start()
    for head in range(heads):
        both(lambda which: far_copy(0, head, which).start())
    own_rate_copy().start()
    for which in range(3):
        first_copy(which).start()
    for group in range(groups):
        for head in range(heads):
            for which in (1, 2, 0):
                local_copy(group, head, which).start()

    @pl.when(early)
    def _():
        for head in range(moved, heads):
            both(lambda which: far_copy(1, head, which).start())

        @pl.when(odd)
        def _():
            for head in range(moved):
                both(lambda which: near_copy(1, 0, head, which).start())

    @pl.when(late)
    def _():
        for at in range(moved):
            visit_copy(at).start()

    @pl.when(even)
    def _():
        for group in range(groups):
            for head in range(heads):
                both(lambda which: near_copy(group, group, head, which).start())

    own_rate_copy().wait()
    for which in range(3):
        first_copy(which).wait()
    low_buf[0] = first_buf[...].astype(jnp.bfloat16)
    for which in range(3):
        final_ref[which] = first_buf[:, which]

    def own_gradients(group, head):
        gradients_of(
            key_buf.at[OWN + group, head],
            value_buf.at[OWN + group, head],
            rate_buf.at[0, group],
            head,
            low_buf.at[group, head],
            own_grad.at[group, head],
        )

    def own_step(head, _):
        local_copy(0, head, 1).wait()
        local_copy(0, head, 2).wait()
        own_gradients(0, head)
        own_copy(0, head).start()
        return 0

    lax.fori_loop(0, heads, own_step, 0)
    rate_copy().wait_recv()

    def sources_of(which, slots, head):
        buf = (key_buf, value_buf)[which]
        return tuple(buf.at[slot, head] for slot in slots)

    def mix_head(group, head, far_slot, near_slot, bias, sources):
        local_copy(group, head, 0).wait()

        @pl.when(jnp.logical_or(group == 1, rank > 0))
        def _():
            both(lambda which: near_copy(group, group, head, which).wait_recv())

        slots = (far_slot, near_slot, OWN + group)
        attend_and_mix(
            bias,
            query_buf.at[group, head],
            sources_of(0, slots, head),
            sources_of(1, slots, head),
            low_buf.at[group, head],
            gain_ref[:, lanes(head)],
            mixed_ref.at[group, :, lanes(head)],
            score_ref,
            sources,
        )

    def send_sums(pair):
        for at in range(2):
            head = 2 * pair + at
            own_copy(1, head).wait_recv()
            sum_buf[head] = own_grad[1, head] + own_got[1, head]
        for at in range(2):
            head = 2 * pair + at

            @pl.when(jnp.logical_or(late, head < moved))
            def _():
                cross_copy(head).start()

    def group_step(group, _):
        lonely = jnp.logical_and(group == 0, rank == 0)
        far_slot = FAR + jnp.where(late, group, 0)
        near_slot = jnp.where(lonely, OWN, NEAR + group)
        bias = (0.0, jnp.where(lonely, BARRED, 0.0).astype(jnp.float32))

        @pl.when(group == 1)
        def _():
            send_sums(heads // 2 - 1)

            def moved_step(at, _):
                head = at

                @pl.when(early)
                def _():
                    visit_copy(at).wait_recv()

                    @pl.when(even)
                    def _():
                        both(lambda which: near_copy(1, 0, head, which).wait_recv())

                    inner_slot = jnp.where(even, NEAR, OWN + 1)
                    barred = (0.0, jnp.where(odd, BARRED, 0.0).astype(jnp.float32))
                    slots = (OWN + 1, inner_slot)
                    attend_part(
                        barred,
                        visit_buf.at[at],
                        sources_of(0, slots, head),
                        sources_of(1, slots, head),
                        part_send_buf.at[at],
                        log_send_buf.at[at],
                        score_ref,
                    )
                    log_copy(at).start()
                    part_copy(at).start()

                @pl.when(late)
                def _():
                    local_copy(1, head, 0).wait()

                    @pl.when(odd)
                    def _():
                        both(lambda which: near_copy(1, 1, head, which).wait_recv())

                    inner_slot = jnp.where(odd, NEAR + 1, OWN + 1)
                    barred = (0.0, jnp.where(even, BARRED, 0.0).astype(jnp.float32))
                    slots = (OWN + 1, inner_slot, OWN + 1)
                    attend_kept(
                        barred,
                        query_buf.at[1, head],
                        sources_of(0, slots, head),
                        sources_of(1, slots, head),
                        low_buf.at[1, head],
                        gain_ref[:, lanes(head)],
                        kept_part.at[at],
                        kept_norm.at[at],
                        kept_log.at[at],
                        score_ref,
                    )

                return 0

            lax.fori_loop(0, moved, moved_step, 0)

        def shares(head):
            return jnp.logical_or(group == 0, jnp.logical_and(late, head >= moved))

        def head_step(head, _):
            shared = shares(head)
            low = low_buf.at[group, head]

            @pl.when(group == 0)
            def _():
                own_copy(0, head).wait_recv()
                sum_buf[head] = own_grad[0, head] + own_got[0, head]

            @pl.when(shared)
            def _():
                both(lambda which: far_copy(group, head, which).wait_recv())

                @pl.when(odd)
                def _():
                    slot = jnp.where(late, group, 1)
                    both(lambda which: relay_copy(group, slot, head, which).start())

                gradients_of(
                    key_buf.at[FAR + group, head],
                    value_buf.at[FAR + group, head],
                    rate_buf.at[1, group],
                    head,
                    low,
                    far_grad.at[group, head],
                )
                swap_copy(group, head).start()

            @pl.when(jnp.logical_and(early, group == 0))
            def _():
                mix_head(0, head, FAR, near_slot, bias, (1, 2))

            last = jnp.logical_and(group == 1, head == heads - 1)

            @pl.when(jnp.where(late, shared, last))
            def _():
                mix_head(group, head, far_slot, near_slot, (0.0, 0.0), (0, 1, 2))

            return 0

        def pair_step(pair, _):
            @pl.when(jnp.logical_and(group == 0, pair > 0))
            def _():
                send_sums(pair - 1)

            lax.fori_loop(2 * pair, 2 * pair + 2, head_step, 0)
            for at in range(2):
                head = 2 * pair + at

                @pl.when(jnp.logical_not(shares(head)))
                def _():
                    cross_copy(head).wait_recv()
                    pass_copy(head).start()

            for at in range(2):
                head = 2 * pair + at

                @pl.when(shares(head))
                def _():
                    swap_copy(group, head).wait_recv()
                    total_buf[at] = sum_buf[head] + (far_grad[group, head] + far_got[group, head])

                @pl.when(jnp.logical_not(shares(head)))
                def _():
                    pass_copy(head).wait_recv()
                    total_buf[at] = sum_buf[head] + cross_buf[head]

            renew_pair(
                total_buf,
                first_buf.at[pl.ds(2 * pair, 2)],
                final_ref.at[:, pl.ds(2 * pair, 2)],
                [step_ref[2 * pair + at] for at in range(2)],
            )

            def after_step(head, _):
                low_buf[1, head] = final_ref[:, head].astype(jnp.bfloat16)
                local_copy(1, head, 1).wait()
                local_copy(1, head, 2).wait()
                own_gradients(1, head)
                own_copy(1, head).start()
                return 0

            def early_step(head, _):
                mix_head(1, head, FAR, NEAR + 1, (0.0, 0.0), (0, 1, 2))
                return 0

            @pl.when(group == 0)
            def _():
                lax.fori_loop(2 * pair, 2 * pair + 2, after_step, 0)

                @pl.when(early)
                def _():
                    stop = jnp.minimum(2 * pair + 2, heads - 1)
                    lax.fori_loop(2 * pair, stop, early_step, 0)

            return 0

        lax.fori_loop(0, heads // 2, pair_step, 0)
        return 0

    lax.fori_loop(0, groups, group_step, 0)

    @pl.when(late)
    def _():
        for at in range(moved):
            log_copy(at).wait_recv()
            part_copy(at).wait_recv()

    rate_copy().wait_send()
    for head in range(heads):
        both(lambda which: far_copy(0, head, which).wait_send())
        for group in range(groups):
            own_copy(group, head).wait_send()
        swap_copy(0, head).wait_send()

    @pl.when(early)
    def _():
        for head in range(moved, heads):
            both(lambda which: far_copy(1, head, which).wait_send())
        for head in range(moved):
            cross_copy(head).wait_send()
        for head in range(heads):
            pass_copy(head).wait_send()
        for at in range(moved):
            log_copy(at).wait_send()
            part_copy(at).wait_send()

        @pl.when(odd)
        def _():
            for head in range(moved):
                both(lambda which: near_copy(1, 0, head, which).wait_send())

    @pl.when(even)
    def _():
        for group in range(groups):
            for head in range(heads):
                both(lambda which: near_copy(group, group, head, which).wait_send())

    @pl.when(odd)
    def _():
        for head in range(heads):
            both(lambda which: relay_copy(0, jnp.where(late, 0, 1), head, which).wait_send())

    @pl.when(late)
    def _():
        for at in range(moved):
            visit_copy(at).wait_send()
        for head in range(heads):
            cross_copy(head).wait_send()
        for head in range(moved):
            pass_copy(head).wait_send()
        for head in range(moved, heads):
            swap_copy(1, head).wait_send()

        @pl.when(odd)
        def _():
            for head in range(moved, heads):
                both(lambda which: relay_copy(1, 1, head, which).wait_send())


def gradients_of(key_ref, value_ref, rate_ref, head, low, out_ref):
    rows = key_ref.shape[0]
    width = low.shape[-1]
    chunk = min(256, rows)
    gate_up = jnp.concatenate([low[0], low[1]], axis=1)
    down = low[2]
    totals = None
    for start in range(0, rows, chunk):
        part = pl.ds(start, chunk)
        keys = key_ref[part, :]
        columns = []
        for at in range(start, start + chunk, HD):
            rates = rate_ref[:, pl.ds(at, HD)]
            place = lax.broadcasted_iota(jnp.int32, rates.shape, 0)
            row = jnp.sum(jnp.where(place == head, rates, 0.0), axis=0, keepdims=True)
            columns.append(jnp.transpose(jnp.broadcast_to(row, (HD, HD))))
        rate = jnp.concatenate(columns, axis=0)
        out_grad = (-rate * value_ref[part, :].astype(jnp.float32)).astype(jnp.bfloat16)
        pre = dot(keys, gate_up, ((1,), (0,)))
        gate_pre, up_pre = pre[:, :width], pre[:, width:]
        squash = sigmoid(gate_pre)
        active = gate_pre * squash
        hidden = (active * up_pre).astype(jnp.bfloat16)
        hidden_grad = dot(out_grad, down, ((1,), (0,)))
        up_grad = (hidden_grad * active).astype(jnp.bfloat16)
        gate_grad = (hidden_grad * up_pre * squash * (1.0 + gate_pre * (1.0 - squash))).astype(
            jnp.bfloat16
        )
        terms = (
            dot(keys, gate_grad, ((0,), (0,))),
            dot(keys, up_grad, ((0,), (0,))),
            dot(out_grad, hidden, ((0,), (0,))),
        )
        for which in range(3):
            if start == 0:
                out_ref[which] = terms[which]
            else:
                out_ref[which] += terms[which]


def renew_pair(gradient_ref, first_ref, current_ref, steps):
    slots = [(at, which) for at in range(2) for which in range(3)]
    matrices = []
    for at, which in slots:
        gradient = gradient_ref[at, which]
        frobenius = jnp.sqrt(jnp.sum(gradient * gradient, keepdims=True))
        matrices.append(gradient / (frobenius + frob_epsilon))
    matrices = sweep_all(matrices)
    for (at, which), matrix in zip(slots, matrices):
        first = first_ref[at, which]
        target = jnp.sqrt(jnp.sum(first * first, axis=0, keepdims=True))
        stepped = current_ref[which, at] - steps[at] * matrix
        length = jnp.sqrt(jnp.sum(stepped * stepped, axis=0, keepdims=True))
        current_ref[which, at] = stepped * (target / (length + column_epsilon))


def sweep_all(matrices):
    for sweep in range(NS_STEPS):
        pairs = [split(matrix) for matrix in matrices]
        grams = [
            dot(
                jnp.concatenate([high, high, rest], axis=1),
                jnp.concatenate([high, rest, high], axis=1),
                ((1,), (1,)),
            )
            for high, rest in pairs
        ]
        polynomials = []
        for gram in grams:
            high, rest = split(gram)
            squared = dot(
                jnp.concatenate([high, high, rest], axis=1),
                jnp.concatenate([high, rest, high], axis=0),
                ((1,), (0,)),
            )
            polynomials.append(coeff_second * gram + coeff_third * squared)
        moved = []
        for polynomial, (high, rest), matrix in zip(polynomials, pairs, matrices):
            poly_high, poly_rest = split(polynomial)
            moved.append(
                coeff_first * matrix
                + dot(
                    jnp.concatenate([poly_high, poly_high, poly_rest], axis=1),
                    jnp.concatenate([high, rest, high], axis=0),
                    ((1,), (0,)),
                )
            )
        matrices = moved
    return matrices


def attend(bias, query_ref, key_refs, value_refs, score_ref, sources, emit):
    rows = query_ref.shape[0]
    tile = min(256, rows)
    per = rows // tile
    span = 2 * per + 1
    factor = math.log2(math.e) / math.sqrt(HD)
    row = lax.broadcasted_iota(jnp.int32, (tile, tile), 0)
    column = lax.broadcasted_iota(jnp.int32, (tile, tile), 1)
    later = column > row

    def fold(op, a):
        folded = a[:, :HD]
        for at in range(HD, tile, HD):
            folded = op(folded, a[:, at : at + HD])
        return folded

    def tiles(block):
        return [at for at in range(span) if (block + at) // per in sources]

    def score(block, at, peak):
        source, place = divmod(block + at, per)
        queries = query_ref[block * tile : (block + 1) * tile, :]
        s = dot(queries, key_refs[source][place * tile : (place + 1) * tile, :], ((1,), (1,)))
        if at == 0:
            s = jnp.where(later, s, EXCLUDED)
        if at == span - 1:
            s = jnp.where(later, EXCLUDED, s)
        score_ref[block % 2, at] = s
        top = fold(jnp.maximum, s)
        if source < 2:
            top = top + bias[source]
        return top if peak is None else jnp.maximum(peak, top)

    peak = None
    for at in tiles(0):
        peak = score(0, at, peak)
    for block in range(per):
        row_max = jnp.max(peak, axis=1, keepdims=True)
        base = (row_max - bias[0], row_max - bias[1], row_max)
        ahead = tiles(block + 1) if block + 1 < per else []
        peak = None
        total = None
        summed = None
        for at in tiles(block):
            if ahead:
                peak = score(block + 1, ahead.pop(0), peak)
            source, place = divmod(block + at, per)
            raised = jnp.exp2((score_ref[block % 2, at] - base[source]) * factor)
            part = fold(jnp.add, raised)
            total = part if total is None else total + part
            o = dot(
                raised.astype(jnp.bfloat16),
                value_refs[source][place * tile : (place + 1) * tile, :],
                ((1,), (0,)),
            )
            summed = o if summed is None else summed + o
        for at in ahead:
            peak = score(block + 1, at, peak)
        weight = jnp.sum(total, axis=1, keepdims=True)
        here = slice(block * tile, (block + 1) * tile)
        emit(here, summed / weight, row_max * factor, weight)


def apply_weights(queries, low, gain):
    width = low.shape[-1]
    gate_up = jnp.concatenate([low[0], low[1]], axis=1)
    pre = dot(queries, gate_up, ((1,), (0,)))
    gate_pre, up_pre = pre[:, :width], pre[:, width:]
    hidden = (gate_pre * sigmoid(gate_pre) * up_pre).astype(jnp.bfloat16)
    applied = dot(hidden, low[2], ((1,), (1,)))
    return (
        applied
        * lax.rsqrt(jnp.mean(applied * applied, axis=1, keepdims=True) + rms_epsilon)
        * gain
    )


def attend_and_mix(
    bias, query_ref, key_refs, value_refs, low, gain, out_ref, score_ref, sources
):
    def emit(here, attended, top, weight):
        normed = apply_weights(query_ref[here, :], low, gain)
        out_ref[here, :] = (normed + attended).astype(jnp.bfloat16)

    attend(bias, query_ref, key_refs, value_refs, score_ref, sources, emit)


def log_sum(top, weight):
    return top + math.log2(math.e) * jnp.log(weight)


def attend_part(bias, query_ref, key_refs, value_refs, part_ref, log_ref, score_ref):
    def emit(here, attended, top, weight):
        part_ref[here, :] = attended.astype(jnp.bfloat16)
        logs = jnp.broadcast_to(log_sum(top, weight), attended.shape)
        for at in range(0, attended.shape[0], HD):
            place = (here.start + at) // HD
            log_ref[place : place + 1, :] = jnp.transpose(logs[at : at + HD])[:1]

    attend(bias, query_ref, key_refs, value_refs, score_ref, (0, 1), emit)


def attend_kept(
    bias, query_ref, key_refs, value_refs, low, gain, part_ref, norm_ref, log_ref, score_ref
):
    def emit(here, attended, top, weight):
        norm_ref[here, :] = apply_weights(query_ref[here, :], low, gain)
        part_ref[here, :] = attended
        log_ref[here, :] = jnp.broadcast_to(log_sum(top, weight), attended.shape)

    attend(bias, query_ref, key_refs, value_refs, score_ref, (1, 2), emit)


def merge_parts(part_ref, norm_ref, log_ref, other_ref, other_log_ref, out_ref):
    for start in range(0, part_ref.shape[0], HD):
        here = slice(start, start + HD)
        place = start // HD
        mine = log_ref[here, :]
        other = jnp.transpose(jnp.broadcast_to(other_log_ref[place : place + 1, :], (HD, HD)))
        top = jnp.maximum(mine, other)
        mine, other = jnp.exp2(mine - top), jnp.exp2(other - top)
        attended = (mine * part_ref[here, :] + other * other_ref[here, :].astype(jnp.float32)) / (
            mine + other
        )
        out_ref[here, :] = (norm_ref[here, :] + attended).astype(jnp.bfloat16)


def finish_kernel(
    moved,
    mixed_ref,
    final_ref,
    part_buf,
    log_buf,
    kept_part,
    kept_norm,
    kept_log,
    mixed_hbm,
    final_hbm,
    merged_buf,
    whole_sem,
    head_sem,
):
    groups, _, features = mixed_ref.shape
    begin = moved * HD
    early = lax.axis_index("seq") < 2

    def final_copy():
        return pltpu.make_async_copy(final_ref, final_hbm, whole_sem.at[0])

    def first_copy():
        return pltpu.make_async_copy(mixed_ref.at[0], mixed_hbm.at[0], whole_sem.at[1])

    def kept_copy():
        part = pl.ds(begin, features - begin)
        return pltpu.make_async_copy(
            mixed_ref.at[1, :, part], mixed_hbm.at[1, :, part], whole_sem.at[2]
        )

    def moved_copy(at):
        return pltpu.make_async_copy(
            merged_buf.at[at], mixed_hbm.at[1, :, pl.ds(at * HD, HD)], head_sem.at[at]
        )

    final_copy().start()
    first_copy().start()
    kept_copy().start()
    for at in range(moved):

        @pl.when(early)
        def _():
            merged_buf[at] = mixed_ref[1, :, at * HD : (at + 1) * HD]

        @pl.when(jnp.logical_not(early))
        def _():
            merge_parts(
                kept_part.at[at],
                kept_norm.at[at],
                kept_log.at[at],
                part_buf.at[at],
                log_buf.at[at],
                merged_buf.at[at],
            )

        moved_copy(at).start()
    final_copy().wait()
    kept_copy().wait()
    first_copy().wait()
    for at in range(moved):
        moved_copy(at).wait()


def whole_layer(queries, keys, values, rates, gate, up, down, steps, gain):
    groups, rows, features = queries.shape
    heads = features // HD
    moved = heads - 1
    width = gate.shape[-1]
    tile = min(256, rows)
    span = 2 * (rows // tile) + 1
    dma = pltpu.SemaphoreType.DMA
    brief, full = jnp.bfloat16, jnp.float32
    matrices = (3, HD, width)
    results = pl.pallas_call(
        functools.partial(layer_kernel, moved),
        in_specs=[pl.BlockSpec(memory_space=pltpu.HBM)] * 7
        + [pl.BlockSpec(memory_space=pltpu.SMEM), pl.BlockSpec(memory_space=pltpu.VMEM)],
        out_specs=[pl.BlockSpec(memory_space=pltpu.VMEM)] * 7,
        out_shape=[
            pltpu.VMEM(queries.shape, brief),
            pltpu.VMEM((3, heads, HD, width), full),
            pltpu.VMEM((moved, rows, HD), brief),
            pltpu.VMEM((moved, rows // HD, HD), full),
            pltpu.VMEM((moved, rows, HD), full),
            pltpu.VMEM((moved, rows, HD), full),
            pltpu.VMEM((moved, rows, HD), full),
        ],
        scratch_shapes=[
            pltpu.VMEM((groups, heads, rows, HD), brief),
            pltpu.VMEM((3 * groups, heads, rows, HD), brief),
            pltpu.VMEM((3 * groups, heads, rows, HD), brief),
            pltpu.VMEM((2, groups, heads, rows), full),
            pltpu.VMEM((heads,) + matrices, full),
            pltpu.VMEM((groups, heads) + matrices, brief),
            pltpu.VMEM((groups, heads) + matrices, full),
            pltpu.VMEM((groups, heads) + matrices, full),
            pltpu.VMEM((groups, heads) + matrices, full),
            pltpu.VMEM((groups, heads) + matrices, full),
            pltpu.VMEM((heads,) + matrices, full),
            pltpu.VMEM((heads,) + matrices, full),
            pltpu.VMEM((2,) + matrices, full),
            pltpu.VMEM((2, span, tile, tile), full),
            pltpu.VMEM((moved, rows, HD), brief),
            pltpu.VMEM((moved, rows, HD), brief),
            pltpu.VMEM((moved, rows // HD, HD), full),
            dma((groups, heads, 3)),
            dma((4,)),
            dma((groups, heads, 2)),
            dma((groups, heads, 2)),
            dma((groups, heads, 2)),
            dma((groups, heads, 2)),
            dma,
            dma,
            dma((groups, heads)),
            dma((groups, heads)),
            dma((groups, heads)),
            dma((groups, heads)),
            dma((heads,)),
            dma((heads,)),
            dma((heads,)),
            dma((heads,)),
            dma((moved,)),
            dma((moved,)),
            dma((moved, 2)),
            dma((moved, 2)),
        ],
        compiler_params=pltpu.CompilerParams(
            collective_id=0, has_side_effects=True, vmem_limit_bytes=VMEM_GRANT
        ),
        name="whole_layer",
    )(queries, keys, values, rates, gate, up, down, steps, gain)
    return pl.pallas_call(
        functools.partial(finish_kernel, moved),
        in_specs=[pl.BlockSpec(memory_space=pltpu.VMEM)] * 7,
        out_specs=[pl.BlockSpec(memory_space=pltpu.HBM)] * 2,
        out_shape=[
            jax.ShapeDtypeStruct(queries.shape, brief),
            jax.ShapeDtypeStruct((3, heads, HD, width), full),
        ],
        scratch_shapes=[pltpu.VMEM((moved, rows, HD), brief), dma((3,)), dma((moved,))],
        compiler_params=pltpu.CompilerParams(vmem_limit_bytes=4 * 2**20),
        cost_estimate=pl.CostEstimate(
            flops=10 * moved * rows * HD,
            bytes_accessed=2 * groups * rows * features + 12 * heads * HD * width,
            transcendentals=2 * moved * rows * HD,
        ),
        name="finish_layer",
    )(*results)


def body(
    query_vectors,
    key_vectors,
    value_vectors,
    token_rates,
    gate_weight,
    up_weight,
    down_weight,
    step_sizes,
    norm_gain,
):
    group_count, tok_rows, feature_width = query_vectors.shape
    head_count = feature_width // HD
    rank = lax.axis_index("seq")
    count = lax.axis_size("seq")
    if count == 4 and group_count == 2 and head_count % 2 == 0:
        return whole_layer(
            query_vectors,
            key_vectors,
            value_vectors,
            token_rates,
            gate_weight,
            up_weight,
            down_weight,
            step_sizes,
            norm_gain[None, :],
        )
    swap = [(i, i ^ 1) for i in range(count)]
    ring = lambda d: [(i, (i + d) % count) for i in range(count)]
    shift = lambda a, route: lax.ppermute(a, "seq", route)
    odd = rank % 2 == 1

    far, near = [], []
    for group in range(group_count):
        far_pair, near_pair = [], []
        for tokens in (key_vectors, value_vectors):
            if group == 0:
                sent = tokens[0]
                route = [(i, i + 2) for i in range(count - 2)]
            else:
                sent = jnp.where(rank >= count - 2, tokens[group - 1], tokens[group])
                route = ring(2)
            far_block = shift(sent, route)
            far_pair.append(far_block)
            near_pair.append(shift(jnp.where(odd, far_block, tokens[group]), swap))
        far.append(far_pair)
        near.append(near_pair)

    spread = head_count == count
    first = jnp.stack([gate_weight, up_weight, down_weight], axis=1)
    rates = jnp.transpose(token_rates, (0, 2, 1))
    gain = norm_gain[None, :]
    bias = jnp.where(rank >= jnp.array([2, 1]), 0.0, EXCLUDED).astype(jnp.float32)
    pair_count = count // 2
    pair, core = rank // 2, rank % 2
    if spread:
        first_mine = lax.dynamic_slice_in_dim(first, rank, 1, 0)
        steps = lax.dynamic_slice_in_dim(step_sizes, rank, 1, 0)
    else:
        first_mine, steps = first, step_sizes
    weights_mine = first_mine
    low = first

    def gather(mine):
        arrived = [mine[0]] + [shift(mine[0], ring(2 * d)) for d in range(1, pair_count)]
        column = jnp.stack(arrived)
        other = shift(column, swap)
        blocks = []
        for head in range(head_count):
            at = (pair - head // 2) % pair_count
            pick = lambda a: lax.dynamic_index_in_dim(a, at, 0, keepdims=False)
            blocks.append(jnp.where(core == head % 2, pick(column), pick(other)))
        return blocks

    mixed = None
    for group in range(group_count):
        gradients = group_gradients(group, key_vectors, value_vectors, rates, low)
        last = group + 1 == group_count
        if spread:
            by_core = gradients.reshape((pair_count, 2) + gradients.shape[1:])
            kept = lax.dynamic_index_in_dim(by_core, core, 1, keepdims=False)
            given = lax.dynamic_index_in_dim(by_core, 1 - core, 1, keepdims=False)
            pair_sum = kept + shift(given, swap)
            block = lambda d: lax.dynamic_slice_in_dim(pair_sum, (pair + d) % pair_count, 1, 0)
            parts = [block(0)] + [shift(block(d), ring(2 * d)) for d in range(1, pair_count)]
        else:
            parts = [lax.psum(gradients, "seq")]
        mixed = mix(
            group,
            bias,
            query_vectors,
            (far[group][0], near[group][0]),
            (far[group][1], near[group][1]),
            key_vectors,
            value_vectors,
            low,
            gain,
            mixed,
        )
        weights_mine, low_mine = renew(parts, first_mine, weights_mine, steps)
        if not spread:
            low = low_mine
        elif not last:
            low = jnp.stack(gather(low_mine))
    if spread:
        final = jnp.stack(gather(weights_mine), axis=1)
    else:
        final = jnp.transpose(weights_mine, (1, 0, 2, 3))
    return (mixed, final)


def solution(mesh):
    return jax.shard_map(
        body,
        mesh=mesh,
        in_specs=(
            P("batch", "seq", "head"),
            P("batch", "seq", "head"),
            P("batch", "seq", "head"),
            P("batch", "head", "seq"),
            P("head", None, None),
            P("head", None, None),
            P("head", None, None),
            P("head"),
            P("head"),
        ),
        out_specs=(P("batch", "seq", "head"), P("batch", "head", None, None)),
        check_vma=False,
    )
```

```python
import functools
import math

import jax
import jax.numpy as jnp
from jax import lax
from jax.experimental import pallas as pl
from jax.experimental.pallas import tpu as pltpu
from jax.sharding import PartitionSpec as P

HD = 128
NS_STEPS = 5

coeff_first = 3.4445
coeff_second = -4.775
coeff_third = 2.0315
frob_epsilon = 1e-07
rms_epsilon = 1e-06
column_epsilon = 1e-06
EXCLUDED = -1e30
BARRED = -3e30
VMEM_GRANT = 51 * 2**20


def dot(a, b, dims):
    return lax.dot_general(a, b, (dims, ((), ())), preferred_element_type=jnp.float32)


def sigmoid(a):
    return 0.5 * jnp.tanh(0.5 * a) + 0.5


def grads_kernel(chunk, key_ref, value_ref, rate_ref, weight_ref, out_ref):
    head = pl.program_id(0)
    width = weight_ref.shape[-1]
    rows = key_ref.shape[0]
    gate_up = jnp.concatenate([weight_ref[0], weight_ref[1]], axis=1).astype(jnp.bfloat16)
    down = weight_ref[2].astype(jnp.bfloat16)
    for start in range(0, rows, chunk):
        part = pl.ds(start, chunk)
        keys = key_ref[part, :]
        rates = rate_ref[part, :]
        lane = lax.broadcasted_iota(jnp.int32, rates.shape, 1)
        rate = jnp.sum(jnp.where(lane == head, rates, 0.0), axis=1, keepdims=True)
        out_grad = (-rate * value_ref[part, :].astype(jnp.float32)).astype(jnp.bfloat16)
        pre = dot(keys, gate_up, ((1,), (0,)))
        gate_pre, up_pre = pre[:, :width], pre[:, width:]
        squash = sigmoid(gate_pre)
        active = gate_pre * squash
        hidden = (active * up_pre).astype(jnp.bfloat16)
        hidden_grad = dot(out_grad, down, ((1,), (0,)))
        up_grad = (hidden_grad * active).astype(jnp.bfloat16)
        gate_grad = (hidden_grad * up_pre * squash * (1.0 + gate_pre * (1.0 - squash))).astype(
            jnp.bfloat16
        )
        terms = (
            dot(keys, gate_grad, ((0,), (0,))),
            dot(keys, up_grad, ((0,), (0,))),
            dot(out_grad, hidden, ((0,), (0,))),
        )
        for which in range(3):
            if start == 0:
                out_ref[which] = terms[which]
            else:
                out_ref[which] += terms[which]


def group_gradients(group, keys, values, rates, weights):
    _, rows, features = keys.shape
    heads = features // HD
    width = weights.shape[-1]
    token_spec = pl.BlockSpec((None, rows, HD), lambda h: (group, 0, h))
    return pl.pallas_call(
        functools.partial(grads_kernel, min(256, rows)),
        grid=(heads,),
        in_specs=[
            token_spec,
            token_spec,
            pl.BlockSpec((None, rows, heads), lambda h: (group, 0, 0)),
            pl.BlockSpec((None, 3, HD, width), lambda h: (h, 0, 0, 0)),
        ],
        out_specs=pl.BlockSpec((None, 3, HD, width), lambda h: (h, 0, 0, 0)),
        out_shape=jax.ShapeDtypeStruct((heads, 3, HD, width), jnp.float32),
        cost_estimate=pl.CostEstimate(
            flops=6 * 2 * 2 * heads * rows * HD * width,
            bytes_accessed=2 * rows * features * 2 + heads * 3 * HD * width * 8,
            transcendentals=heads * rows * width,
        ),
        name="group_gradients",
    )(keys, values, rates, weights)


def split(a):
    high = a.astype(jnp.bfloat16)
    return high, (a - high.astype(jnp.float32)).astype(jnp.bfloat16)


def renew_kernel(parts, *refs):
    grad_refs = refs[:parts]
    first_ref, weight_ref, step_ref, new_ref, low_ref = refs[parts:]
    step = step_ref[pl.program_id(0)]
    matrices = []
    for which in range(3):
        gradient = grad_refs[0][which]
        for ref in grad_refs[1:]:
            gradient = gradient + ref[which]
        frobenius = jnp.sqrt(jnp.sum(gradient * gradient, keepdims=True))
        matrices.append(gradient / (frobenius + frob_epsilon))
    for sweep in range(NS_STEPS):
        pairs = [split(matrix) for matrix in matrices]
        grams = [
            dot(
                jnp.concatenate([high, high, rest], axis=1),
                jnp.concatenate([high, rest, high], axis=1),
                ((1,), (1,)),
            )
            for high, rest in pairs
        ]
        polynomials = []
        for gram in grams:
            high, rest = split(gram)
            squared = dot(
                jnp.concatenate([high, high, rest], axis=1),
                jnp.concatenate([high, rest, high], axis=0),
                ((1,), (0,)),
            )
            polynomials.append(coeff_second * gram + coeff_third * squared)
        moved = []
        for polynomial, (high, rest), matrix in zip(polynomials, pairs, matrices):
            poly_high, poly_rest = split(polynomial)
            moved.append(
                coeff_first * matrix
                + dot(
                    jnp.concatenate([poly_high, poly_high, poly_rest], axis=1),
                    jnp.concatenate([high, rest, high], axis=0),
                    ((1,), (0,)),
                )
            )
        matrices = moved
    for which in range(3):
        first = first_ref[which]
        target = jnp.sqrt(jnp.sum(first * first, axis=0, keepdims=True))
        stepped = weight_ref[which] - step * matrices[which]
        length = jnp.sqrt(jnp.sum(stepped * stepped, axis=0, keepdims=True))
        renewed = stepped * (target / (length + column_epsilon))
        new_ref[which] = renewed
        low_ref[which] = renewed.astype(jnp.bfloat16)


def renew(gradients, first, weights, steps):
    heads, _, _, width = weights.shape
    spec = pl.BlockSpec((None, 3, HD, width), lambda h: (h, 0, 0, 0))
    return pl.pallas_call(
        functools.partial(renew_kernel, len(gradients)),
        grid=(heads,),
        in_specs=[spec] * (len(gradients) + 2) + [pl.BlockSpec(memory_space=pltpu.SMEM)],
        out_specs=[spec, spec],
        out_shape=[
            jax.ShapeDtypeStruct(weights.shape, jnp.float32),
            jax.ShapeDtypeStruct(weights.shape, jnp.bfloat16),
        ],
        cost_estimate=pl.CostEstimate(
            flops=heads * 3 * NS_STEPS * 10 * HD * HD * width * 4,
            bytes_accessed=heads * 3 * HD * width * 20,
            transcendentals=0,
        ),
        name="renew_weights",
    )(*gradients, first, weights, steps)


def mix_kernel(
    tile,
    guarded,
    bias_ref,
    query_ref,
    key_far,
    key_near,
    key_own,
    value_far,
    value_near,
    value_own,
    weight_ref,
    gain_ref,
    *rest,
):
    out_ref, score_ref = rest[-2:]
    rows = query_ref.shape[0]
    width = weight_ref.shape[-1]
    per = rows // tile
    blocks = per
    span = 2 * per + 1
    factor = math.log2(math.e) / math.sqrt(HD)
    key_refs = (key_far, key_near, key_own)
    value_refs = (value_far, value_near, value_own)
    gate_up = jnp.concatenate([weight_ref[0], weight_ref[1]], axis=1).astype(jnp.bfloat16)
    down = weight_ref[2].astype(jnp.bfloat16)
    gain = gain_ref[...]
    row = lax.broadcasted_iota(jnp.int32, (tile, tile), 0)
    column = lax.broadcasted_iota(jnp.int32, (tile, tile), 1)
    later = column > row

    def fold(op, a):
        folded = a[:, :HD]
        for at in range(HD, tile, HD):
            folded = op(folded, a[:, at : at + HD])
        return folded

    def score(block, at, peak):
        source, place = divmod(block + at, per)
        queries = query_ref[block * tile : (block + 1) * tile, :]
        s = dot(queries, key_refs[source][place * tile : (place + 1) * tile, :], ((1,), (1,)))
        if at == 0:
            s = jnp.where(later, s, EXCLUDED)
        if at == span - 1:
            s = jnp.where(later, EXCLUDED, s)
        if guarded and source < 2:
            s = s + bias_ref[source]
        score_ref[block % 2, at] = s
        top = fold(jnp.maximum, s)
        return top if peak is None else jnp.maximum(peak, top)

    peak = None
    for at in range(span):
        peak = score(0, at, peak)
    for block in range(blocks):
        row_max = jnp.max(peak, axis=1, keepdims=True)
        peak = None
        total = None
        summed = None
        for at in range(span):
            if block + 1 < blocks:
                peak = score(block + 1, at, peak)
            raised = jnp.exp2((score_ref[block % 2, at] - row_max) * factor)
            part = fold(jnp.add, raised)
            total = part if total is None else total + part
            source, place = divmod(block + at, per)
            o = dot(
                raised.astype(jnp.bfloat16),
                value_refs[source][place * tile : (place + 1) * tile, :],
                ((1,), (0,)),
            )
            summed = o if summed is None else summed + o
        attended = summed / jnp.sum(total, axis=1, keepdims=True)
        here = slice(block * tile, (block + 1) * tile)
        pre = dot(query_ref[here, :], gate_up, ((1,), (0,)))
        gate_pre, up_pre = pre[:, :width], pre[:, width:]
        hidden = (gate_pre * sigmoid(gate_pre) * up_pre).astype(jnp.bfloat16)
        applied = dot(hidden, down, ((1,), (1,)))
        normed = (
            applied
            * lax.rsqrt(jnp.mean(applied * applied, axis=1, keepdims=True) + rms_epsilon)
            * gain
        )
        out_ref[here, :] = (normed + attended).astype(jnp.bfloat16)


def mix(group, bias, queries, keys, values, own_keys, own_values, weights, gain, earlier):
    group_count, rows, features = queries.shape
    heads = features // HD
    width = weights.shape[-1]
    tile = min(256, rows)
    own = pl.BlockSpec((None, rows, HD), lambda h: (group, 0, h))
    passed = pl.BlockSpec((rows, HD), lambda h: (0, h))
    operands = [bias, queries, *keys, own_keys, *values, own_values, weights, gain]
    in_specs = [
        pl.BlockSpec(memory_space=pltpu.SMEM),
        own,
        passed,
        passed,
        own,
        passed,
        passed,
        own,
        pl.BlockSpec((None, 3, HD, width), lambda h: (h, 0, 0, 0)),
        pl.BlockSpec((1, HD), lambda h: (0, h)),
    ]
    aliases = {}
    if earlier is not None:
        aliases = {len(operands): 0}
        operands.append(earlier)
        in_specs.append(pl.BlockSpec(memory_space=pl.ANY))
    return pl.pallas_call(
        functools.partial(mix_kernel, tile, group == 0),
        grid=(heads,),
        in_specs=in_specs,
        out_specs=own,
        out_shape=jax.ShapeDtypeStruct(queries.shape, jnp.bfloat16),
        scratch_shapes=[pltpu.VMEM((2, 2 * rows // tile + 1, tile, tile), jnp.float32)],
        input_output_aliases=aliases,
        cost_estimate=pl.CostEstimate(
            flops=heads * rows * (2 * rows + tile) * HD * 4 * 2,
            bytes_accessed=8 * rows * features * 2,
            transcendentals=heads * rows * (2 * rows + tile),
        ),
        name="attend_and_mix",
    )(*operands)


def layer_kernel(
    moved,
    query_hbm,
    key_hbm,
    value_hbm,
    rate_hbm,
    gate_hbm,
    up_hbm,
    down_hbm,
    step_ref,
    gain_ref,
    mixed_ref,
    final_ref,
    part_buf,
    log_buf,
    kept_part,
    kept_norm,
    kept_log,
    query_buf,
    key_buf,
    value_buf,
    rate_buf,
    first_buf,
    low_buf,
    own_grad,
    own_got,
    far_grad,
    far_got,
    sum_buf,
    cross_buf,
    total_buf,
    score_ref,
    visit_buf,
    part_send_buf,
    log_send_buf,
    local_sem,
    small_sem,
    far_send,
    far_recv,
    near_send,
    near_recv,
    rate_send,
    rate_recv,
    own_send,
    own_recv,
    swap_send,
    swap_recv,
    cross_send,
    cross_recv,
    pass_send,
    pass_recv,
    visit_send,
    visit_recv,
    part_send,
    part_recv,
):
    groups, heads, rows, _ = query_buf.shape
    rank = lax.axis_index("seq")
    partner = rank + 1 - 2 * (rank % 2)
    count = lax.axis_size("seq")
    across = (rank + count // 2) % count
    core = rank % 2
    odd = core == 1
    even = core == 0
    early = rank < count // 2
    late = rank >= count // 2
    OWN, FAR, NEAR = 0, groups, 2 * groups
    mesh_ids = pl.DeviceIdType.MESH
    slab = HD // 2

    def lanes(head):
        return pl.ds(pl.multiple_of(head * HD, HD), HD)

    def remote(src, dst, send, recv, to):
        return pltpu.make_async_remote_copy(
            src_ref=src,
            dst_ref=dst,
            send_sem=send,
            recv_sem=recv,
            device_id={"seq": to},
            device_id_type=mesh_ids,
        )

    def far_copy(group, head, which):
        source, target = ((key_hbm, key_buf), (value_hbm, value_buf))[which]
        return remote(
            source.at[group, :, lanes(head)],
            target.at[FAR + group, head],
            far_send.at[group, head, which],
            far_recv.at[group, head, which],
            across,
        )

    def near_copy(group, slot, head, which):
        source, target = ((key_hbm, key_buf), (value_hbm, value_buf))[which]
        return remote(
            source.at[group, :, lanes(head)],
            target.at[NEAR + slot, head],
            near_send.at[slot, head, which],
            near_recv.at[slot, head, which],
            partner,
        )

    def relay_copy(group, slot, head, which):
        target = (key_buf, value_buf)[which]
        return remote(
            target.at[FAR + group, head],
            target.at[NEAR + slot, head],
            near_send.at[slot, head, which],
            near_recv.at[slot, head, which],
            partner,
        )

    def rate_copy(group):
        return remote(
            rate_hbm.at[group],
            rate_buf.at[1, group],
            rate_send.at[group],
            rate_recv.at[group],
            across,
        )

    def local_copy(group, head, which):
        source = (query_hbm, key_hbm, value_hbm)[which]
        if which == 0:
            target = query_buf.at[group, head]
        else:
            target = (key_buf, value_buf)[which - 1].at[OWN + group, head]
        return pltpu.make_async_copy(
            source.at[group, :, lanes(head)], target, local_sem.at[group, head, which]
        )

    def first_copy(which):
        source = (gate_hbm, up_hbm, down_hbm)[which]
        return pltpu.make_async_copy(source, first_buf.at[:, which], small_sem.at[which])

    def own_rate_copy():
        return pltpu.make_async_copy(rate_hbm, rate_buf.at[0], small_sem.at[3])

    def own_copy(group, head):
        return remote(
            own_grad.at[group, head],
            own_got.at[group, head],
            own_send.at[group, head],
            own_recv.at[group, head],
            partner,
        )

    def swap_copy(group, head):
        return remote(
            far_grad.at[group, head],
            far_got.at[group, head],
            swap_send.at[group, head],
            swap_recv.at[group, head],
            partner,
        )

    def cross_copy(head):
        part = pl.ds(pl.multiple_of(core * slab, slab), slab)
        return remote(
            sum_buf.at[head, :, part],
            cross_buf.at[head, :, part],
            cross_send.at[head],
            cross_recv.at[head],
            across,
        )

    def pass_copy(head):
        part = pl.ds(pl.multiple_of(core * slab, slab), slab)
        return remote(
            cross_buf.at[head, :, part],
            cross_buf.at[head, :, part],
            pass_send.at[head],
            pass_recv.at[head],
            partner,
        )

    def visit_copy(at):
        return remote(
            query_hbm.at[1, :, lanes(at)],
            visit_buf.at[at],
            visit_send.at[at],
            visit_recv.at[at],
            across,
        )

    def part_copy(at):
        return remote(
            part_send_buf.at[at], part_buf.at[at], part_send.at[at, 0], part_recv.at[at, 0], across
        )

    def log_copy(at):
        return remote(
            log_send_buf.at[at], log_buf.at[at], part_send.at[at, 1], part_recv.at[at, 1], across
        )

    def both(make):
        for which in range(2):
            make(which)

    barrier = pltpu.get_barrier_semaphore()
    for peer in (partner, across):
        pl.semaphore_signal(barrier, inc=1, device_id={"seq": peer}, device_id_type=mesh_ids)
    pl.semaphore_wait(barrier, 2)

    rate_copy(0).start()
    for head in range(heads):
        both(lambda which: far_copy(0, head, which).start())
    own_rate_copy().start()
    for which in range(3):
        first_copy(which).start()
    for group in range(groups):
        for head in range(heads):
            for which in (1, 2, 0):
                local_copy(group, head, which).start()

    @pl.when(early)
    def _():
        rate_copy(1).start()
        for head in range(moved, heads):
            both(lambda which: far_copy(1, head, which).start())

        @pl.when(odd)
        def _():
            for head in range(moved):
                both(lambda which: near_copy(1, 0, head, which).start())

    @pl.when(late)
    def _():
        for at in range(moved):
            visit_copy(at).start()

    @pl.when(even)
    def _():
        for group in range(groups):
            for head in range(heads):
                both(lambda which: near_copy(group, group, head, which).start())

    own_rate_copy().wait()
    for which in range(3):
        first_copy(which).wait()
    low_buf[0] = first_buf[...].astype(jnp.bfloat16)
    for which in range(3):
        final_ref[which] = first_buf[:, which]

    def own_gradients(group, head):
        gradients_of(
            key_buf.at[OWN + group, head],
            value_buf.at[OWN + group, head],
            rate_buf.at[0, group],
            head,
            low_buf.at[group, head],
            own_grad.at[group, head],
        )

    def own_step(head, _):
        local_copy(0, head, 1).wait()
        local_copy(0, head, 2).wait()
        own_gradients(0, head)
        own_copy(0, head).start()
        return 0

    lax.fori_loop(0, heads, own_step, 0)
    rate_copy(0).wait_recv()

    def sources_of(which, slots, head):
        buf = (key_buf, value_buf)[which]
        return tuple(buf.at[slot, head] for slot in slots)

    def mix_head(group, head, far_slot, near_slot, bias, sources):
        local_copy(group, head, 0).wait()

        @pl.when(jnp.logical_or(group == 1, rank > 0))
        def _():
            both(lambda which: near_copy(group, group, head, which).wait_recv())

        slots = (far_slot, near_slot, OWN + group)
        attend_and_mix(
            bias,
            query_buf.at[group, head],
            sources_of(0, slots, head),
            sources_of(1, slots, head),
            low_buf.at[group, head],
            gain_ref[:, lanes(head)],
            mixed_ref.at[group, :, lanes(head)],
            score_ref,
            sources,
        )

    def send_sums(pair):
        for at in range(2):
            head = 2 * pair + at
            own_copy(1, head).wait_recv()
            sum_buf[head] = own_grad[1, head] + own_got[1, head]
        for at in range(2):
            head = 2 * pair + at

            @pl.when(jnp.logical_or(late, head < moved))
            def _():
                cross_copy(head).start()

    def group_step(group, _):
        lonely = jnp.logical_and(group == 0, rank == 0)
        far_slot = FAR + jnp.where(late, group, 0)
        near_slot = jnp.where(lonely, OWN, NEAR + group)
        bias = (0.0, jnp.where(lonely, BARRED, 0.0).astype(jnp.float32))

        @pl.when(group == 1)
        def _():
            send_sums(heads // 2 - 1)

            def moved_step(at, _):
                head = at

                @pl.when(early)
                def _():
                    visit_copy(at).wait_recv()

                    @pl.when(even)
                    def _():
                        both(lambda which: near_copy(1, 0, head, which).wait_recv())

                    inner_slot = jnp.where(even, NEAR, OWN + 1)
                    barred = (0.0, jnp.where(odd, BARRED, 0.0).astype(jnp.float32))
                    slots = (OWN + 1, inner_slot)
                    attend_part(
                        barred,
                        visit_buf.at[at],
                        sources_of(0, slots, head),
                        sources_of(1, slots, head),
                        part_send_buf.at[at],
                        log_send_buf.at[at],
                        score_ref,
                    )
                    log_copy(at).start()
                    part_copy(at).start()

                @pl.when(late)
                def _():
                    local_copy(1, head, 0).wait()

                    @pl.when(at == 0)
                    def _():
                        rate_copy(1).wait_recv()

                    @pl.when(odd)
                    def _():
                        both(lambda which: near_copy(1, 1, head, which).wait_recv())

                    inner_slot = jnp.where(odd, NEAR + 1, OWN + 1)
                    barred = (0.0, jnp.where(even, BARRED, 0.0).astype(jnp.float32))
                    slots = (OWN + 1, inner_slot, OWN + 1)
                    attend_kept(
                        barred,
                        query_buf.at[1, head],
                        sources_of(0, slots, head),
                        sources_of(1, slots, head),
                        low_buf.at[1, head],
                        gain_ref[:, lanes(head)],
                        kept_part.at[at],
                        kept_norm.at[at],
                        kept_log.at[at],
                        score_ref,
                    )

                return 0

            lax.fori_loop(0, moved, moved_step, 0)

            @pl.when(early)
            def _():
                mix_head(1, heads - 1, FAR, NEAR + 1, (0.0, 0.0), (0, 1, 2))

        def shares(head):
            return jnp.logical_or(group == 0, jnp.logical_and(late, head >= moved))

        def head_step(head, _):
            shared = shares(head)
            low = low_buf.at[group, head]

            @pl.when(group == 0)
            def _():
                own_copy(0, head).wait_recv()
                sum_buf[head] = own_grad[0, head] + own_got[0, head]

            @pl.when(shared)
            def _():
                both(lambda which: far_copy(group, head, which).wait_recv())

                @pl.when(odd)
                def _():
                    slot = jnp.where(late, group, 1)
                    both(lambda which: relay_copy(group, slot, head, which).start())

                gradients_of(
                    key_buf.at[FAR + group, head],
                    value_buf.at[FAR + group, head],
                    rate_buf.at[1, group],
                    head,
                    low,
                    far_grad.at[group, head],
                )
                swap_copy(group, head).start()

            @pl.when(jnp.logical_and(early, group == 0))
            def _():
                mix_head(0, head, FAR, near_slot, bias, (1, 2))

            @pl.when(jnp.logical_and(late, shared))
            def _():
                mix_head(group, head, far_slot, near_slot, (0.0, 0.0), (0, 1, 2))

            return 0

        def pair_step(pair, _):
            @pl.when(jnp.logical_and(group == 0, pair > 0))
            def _():
                send_sums(pair - 1)

            lax.fori_loop(2 * pair, 2 * pair + 2, head_step, 0)
            for at in range(2):
                head = 2 * pair + at

                @pl.when(jnp.logical_not(shares(head)))
                def _():
                    cross_copy(head).wait_recv()
                    pass_copy(head).start()

            for at in range(2):
                head = 2 * pair + at

                @pl.when(shares(head))
                def _():
                    swap_copy(group, head).wait_recv()
                    total_buf[at] = sum_buf[head] + (far_grad[group, head] + far_got[group, head])

                @pl.when(jnp.logical_not(shares(head)))
                def _():
                    pass_copy(head).wait_recv()
                    total_buf[at] = sum_buf[head] + cross_buf[head]

            renew_pair(
                total_buf,
                first_buf.at[pl.ds(2 * pair, 2)],
                final_ref.at[:, pl.ds(2 * pair, 2)],
                [step_ref[2 * pair + at] for at in range(2)],
            )

            def after_step(head, _):
                low_buf[1, head] = final_ref[:, head].astype(jnp.bfloat16)
                local_copy(1, head, 1).wait()
                local_copy(1, head, 2).wait()
                own_gradients(1, head)
                own_copy(1, head).start()
                return 0

            def early_step(head, _):
                mix_head(1, head, FAR, NEAR + 1, (0.0, 0.0), (0, 1, 2))
                return 0

            @pl.when(group == 0)
            def _():
                lax.fori_loop(2 * pair, 2 * pair + 2, after_step, 0)

                @pl.when(early)
                def _():
                    stop = jnp.minimum(2 * pair + 2, heads - 1)
                    lax.fori_loop(2 * pair, stop, early_step, 0)

            return 0

        lax.fori_loop(0, heads // 2, pair_step, 0)
        return 0

    lax.fori_loop(0, groups, group_step, 0)

    @pl.when(late)
    def _():
        for at in range(moved):
            log_copy(at).wait_recv()
            part_copy(at).wait_recv()

    rate_copy(0).wait_send()
    for head in range(heads):
        both(lambda which: far_copy(0, head, which).wait_send())
        for group in range(groups):
            own_copy(group, head).wait_send()
        swap_copy(0, head).wait_send()

    @pl.when(early)
    def _():
        rate_copy(1).wait_send()
        for head in range(moved, heads):
            both(lambda which: far_copy(1, head, which).wait_send())
        for head in range(moved):
            cross_copy(head).wait_send()
        for head in range(heads):
            pass_copy(head).wait_send()
        for at in range(moved):
            log_copy(at).wait_send()
            part_copy(at).wait_send()

        @pl.when(odd)
        def _():
            for head in range(moved):
                both(lambda which: near_copy(1, 0, head, which).wait_send())

    @pl.when(even)
    def _():
        for group in range(groups):
            for head in range(heads):
                both(lambda which: near_copy(group, group, head, which).wait_send())

    @pl.when(odd)
    def _():
        for head in range(heads):
            both(lambda which: relay_copy(0, jnp.where(late, 0, 1), head, which).wait_send())

    @pl.when(late)
    def _():
        for at in range(moved):
            visit_copy(at).wait_send()
        for head in range(heads):
            cross_copy(head).wait_send()
        for head in range(moved):
            pass_copy(head).wait_send()
        for head in range(moved, heads):
            swap_copy(1, head).wait_send()

        @pl.when(odd)
        def _():
            for head in range(moved, heads):
                both(lambda which: relay_copy(1, 1, head, which).wait_send())


def gradients_of(key_ref, value_ref, rate_ref, head, low, out_ref):
    rows = key_ref.shape[0]
    width = low.shape[-1]
    chunk = min(256, rows)
    gate_up = jnp.concatenate([low[0], low[1]], axis=1)
    down = low[2]
    totals = None
    for start in range(0, rows, chunk):
        part = pl.ds(start, chunk)
        keys = key_ref[part, :]
        columns = []
        for at in range(start, start + chunk, HD):
            rates = rate_ref[:, pl.ds(at, HD)]
            place = lax.broadcasted_iota(jnp.int32, rates.shape, 0)
            row = jnp.sum(jnp.where(place == head, rates, 0.0), axis=0, keepdims=True)
            columns.append(jnp.transpose(jnp.broadcast_to(row, (HD, HD))))
        rate = jnp.concatenate(columns, axis=0)
        out_grad = (-rate * value_ref[part, :].astype(jnp.float32)).astype(jnp.bfloat16)
        pre = dot(keys, gate_up, ((1,), (0,)))
        gate_pre, up_pre = pre[:, :width], pre[:, width:]
        squash = sigmoid(gate_pre)
        active = gate_pre * squash
        hidden = (active * up_pre).astype(jnp.bfloat16)
        hidden_grad = dot(out_grad, down, ((1,), (0,)))
        up_grad = (hidden_grad * active).astype(jnp.bfloat16)
        gate_grad = (hidden_grad * up_pre * squash * (1.0 + gate_pre * (1.0 - squash))).astype(
            jnp.bfloat16
        )
        terms = (
            dot(keys, gate_grad, ((0,), (0,))),
            dot(keys, up_grad, ((0,), (0,))),
            dot(out_grad, hidden, ((0,), (0,))),
        )
        for which in range(3):
            if start == 0:
                out_ref[which] = terms[which]
            else:
                out_ref[which] += terms[which]


def renew_pair(gradient_ref, first_ref, current_ref, steps):
    slots = [(at, which) for at in range(2) for which in range(3)]
    matrices = []
    for at, which in slots:
        gradient = gradient_ref[at, which]
        frobenius = jnp.sqrt(jnp.sum(gradient * gradient, keepdims=True))
        matrices.append(gradient / (frobenius + frob_epsilon))
    matrices = sweep_all(matrices)
    for (at, which), matrix in zip(slots, matrices):
        first = first_ref[at, which]
        target = jnp.sqrt(jnp.sum(first * first, axis=0, keepdims=True))
        stepped = current_ref[which, at] - steps[at] * matrix
        length = jnp.sqrt(jnp.sum(stepped * stepped, axis=0, keepdims=True))
        current_ref[which, at] = stepped * (target / (length + column_epsilon))


def sweep_all(matrices):
    for sweep in range(NS_STEPS):
        pairs = [split(matrix) for matrix in matrices]
        grams = [
            dot(
                jnp.concatenate([high, high, rest], axis=1),
                jnp.concatenate([high, rest, high], axis=1),
                ((1,), (1,)),
            )
            for high, rest in pairs
        ]
        polynomials = []
        for gram in grams:
            high, rest = split(gram)
            squared = dot(
                jnp.concatenate([high, high, rest], axis=1),
                jnp.concatenate([high, rest, high], axis=0),
                ((1,), (0,)),
            )
            polynomials.append(coeff_second * gram + coeff_third * squared)
        moved = []
        for polynomial, (high, rest), matrix in zip(polynomials, pairs, matrices):
            poly_high, poly_rest = split(polynomial)
            moved.append(
                coeff_first * matrix
                + dot(
                    jnp.concatenate([poly_high, poly_high, poly_rest], axis=1),
                    jnp.concatenate([high, rest, high], axis=0),
                    ((1,), (0,)),
                )
            )
        matrices = moved
    return matrices


def attend(bias, query_ref, key_refs, value_refs, score_ref, sources, emit):
    rows = query_ref.shape[0]
    tile = min(256, rows)
    per = rows // tile
    span = 2 * per + 1
    factor = math.log2(math.e) / math.sqrt(HD)
    row = lax.broadcasted_iota(jnp.int32, (tile, tile), 0)
    column = lax.broadcasted_iota(jnp.int32, (tile, tile), 1)
    later = column > row

    def fold(op, a):
        folded = a[:, :HD]
        for at in range(HD, tile, HD):
            folded = op(folded, a[:, at : at + HD])
        return folded

    def tiles(block):
        return [at for at in range(span) if (block + at) // per in sources]

    def score(block, at, peak):
        source, place = divmod(block + at, per)
        queries = query_ref[block * tile : (block + 1) * tile, :]
        s = dot(queries, key_refs[source][place * tile : (place + 1) * tile, :], ((1,), (1,)))
        if at == 0:
            s = jnp.where(later, s, EXCLUDED)
        if at == span - 1:
            s = jnp.where(later, EXCLUDED, s)
        score_ref[block % 2, at] = s
        top = fold(jnp.maximum, s)
        if source < 2:
            top = top + bias[source]
        return top if peak is None else jnp.maximum(peak, top)

    peak = None
    for at in tiles(0):
        peak = score(0, at, peak)
    for block in range(per):
        row_max = jnp.max(peak, axis=1, keepdims=True)
        base = (row_max - bias[0], row_max - bias[1], row_max)
        ahead = tiles(block + 1) if block + 1 < per else []
        peak = None
        total = None
        summed = None
        for at in tiles(block):
            if ahead:
                peak = score(block + 1, ahead.pop(0), peak)
            source, place = divmod(block + at, per)
            raised = jnp.exp2((score_ref[block % 2, at] - base[source]) * factor)
            part = fold(jnp.add, raised)
            total = part if total is None else total + part
            o = dot(
                raised.astype(jnp.bfloat16),
                value_refs[source][place * tile : (place + 1) * tile, :],
                ((1,), (0,)),
            )
            summed = o if summed is None else summed + o
        for at in ahead:
            peak = score(block + 1, at, peak)
        weight = jnp.sum(total, axis=1, keepdims=True)
        here = slice(block * tile, (block + 1) * tile)
        emit(here, summed / weight, row_max * factor, weight)


def apply_weights(queries, low, gain):
    width = low.shape[-1]
    gate_up = jnp.concatenate([low[0], low[1]], axis=1)
    pre = dot(queries, gate_up, ((1,), (0,)))
    gate_pre, up_pre = pre[:, :width], pre[:, width:]
    hidden = (gate_pre * sigmoid(gate_pre) * up_pre).astype(jnp.bfloat16)
    applied = dot(hidden, low[2], ((1,), (1,)))
    return (
        applied
        * lax.rsqrt(jnp.mean(applied * applied, axis=1, keepdims=True) + rms_epsilon)
        * gain
    )


def attend_and_mix(
    bias, query_ref, key_refs, value_refs, low, gain, out_ref, score_ref, sources
):
    def emit(here, attended, top, weight):
        normed = apply_weights(query_ref[here, :], low, gain)
        out_ref[here, :] = (normed + attended).astype(jnp.bfloat16)

    attend(bias, query_ref, key_refs, value_refs, score_ref, sources, emit)


def log_sum(top, weight):
    return top + math.log2(math.e) * jnp.log(weight)


def attend_part(bias, query_ref, key_refs, value_refs, part_ref, log_ref, score_ref):
    def emit(here, attended, top, weight):
        part_ref[here, :] = attended.astype(jnp.bfloat16)
        logs = jnp.broadcast_to(log_sum(top, weight), attended.shape)
        for at in range(0, attended.shape[0], HD):
            place = (here.start + at) // HD
            log_ref[place : place + 1, :] = jnp.transpose(logs[at : at + HD])[:1]

    attend(bias, query_ref, key_refs, value_refs, score_ref, (0, 1), emit)


def attend_kept(
    bias, query_ref, key_refs, value_refs, low, gain, part_ref, norm_ref, log_ref, score_ref
):
    def emit(here, attended, top, weight):
        norm_ref[here, :] = apply_weights(query_ref[here, :], low, gain)
        part_ref[here, :] = attended
        log_ref[here, :] = jnp.broadcast_to(log_sum(top, weight), attended.shape)

    attend(bias, query_ref, key_refs, value_refs, score_ref, (1, 2), emit)


def merge_parts(part_ref, norm_ref, log_ref, other_ref, other_log_ref, out_ref):
    for start in range(0, part_ref.shape[0], HD):
        here = slice(start, start + HD)
        place = start // HD
        mine = log_ref[here, :]
        other = jnp.transpose(jnp.broadcast_to(other_log_ref[place : place + 1, :], (HD, HD)))
        top = jnp.maximum(mine, other)
        mine, other = jnp.exp2(mine - top), jnp.exp2(other - top)
        attended = (mine * part_ref[here, :] + other * other_ref[here, :].astype(jnp.float32)) / (
            mine + other
        )
        out_ref[here, :] = (norm_ref[here, :] + attended).astype(jnp.bfloat16)


def finish_kernel(
    moved,
    mixed_ref,
    final_ref,
    part_buf,
    log_buf,
    kept_part,
    kept_norm,
    kept_log,
    mixed_hbm,
    final_hbm,
    merged_buf,
    whole_sem,
    head_sem,
):
    groups, _, features = mixed_ref.shape
    begin = moved * HD
    early = lax.axis_index("seq") < lax.axis_size("seq") // 2

    def final_copy():
        return pltpu.make_async_copy(final_ref, final_hbm, whole_sem.at[0])

    def first_copy():
        return pltpu.make_async_copy(mixed_ref.at[0], mixed_hbm.at[0], whole_sem.at[1])

    def kept_copy():
        part = pl.ds(begin, features - begin)
        return pltpu.make_async_copy(
            mixed_ref.at[1, :, part], mixed_hbm.at[1, :, part], whole_sem.at[2]
        )

    def moved_copy(at):
        return pltpu.make_async_copy(
            merged_buf.at[at], mixed_hbm.at[1, :, pl.ds(at * HD, HD)], head_sem.at[at]
        )

    final_copy().start()
    first_copy().start()
    kept_copy().start()
    for at in range(moved):

        @pl.when(early)
        def _():
            merged_buf[at] = mixed_ref[1, :, at * HD : (at + 1) * HD]

        @pl.when(jnp.logical_not(early))
        def _():
            merge_parts(
                kept_part.at[at],
                kept_norm.at[at],
                kept_log.at[at],
                part_buf.at[at],
                log_buf.at[at],
                merged_buf.at[at],
            )

        moved_copy(at).start()
    final_copy().wait()
    kept_copy().wait()
    first_copy().wait()
    for at in range(moved):
        moved_copy(at).wait()


def whole_layer(queries, keys, values, rates, gate, up, down, steps, gain):
    groups, rows, features = queries.shape
    heads = features // HD
    moved = heads - 1
    width = gate.shape[-1]
    tile = min(256, rows)
    span = 2 * (rows // tile) + 1
    dma = pltpu.SemaphoreType.DMA
    brief, full = jnp.bfloat16, jnp.float32
    matrices = (3, HD, width)
    results = pl.pallas_call(
        functools.partial(layer_kernel, moved),
        in_specs=[pl.BlockSpec(memory_space=pltpu.HBM)] * 7
        + [pl.BlockSpec(memory_space=pltpu.SMEM), pl.BlockSpec(memory_space=pltpu.VMEM)],
        out_specs=[pl.BlockSpec(memory_space=pltpu.VMEM)] * 7,
        out_shape=[
            pltpu.VMEM(queries.shape, brief),
            pltpu.VMEM((3, heads, HD, width), full),
            pltpu.VMEM((moved, rows, HD), brief),
            pltpu.VMEM((moved, rows // HD, HD), full),
            pltpu.VMEM((moved, rows, HD), full),
            pltpu.VMEM((moved, rows, HD), full),
            pltpu.VMEM((moved, rows, HD), full),
        ],
        scratch_shapes=[
            pltpu.VMEM((groups, heads, rows, HD), brief),
            pltpu.VMEM((3 * groups, heads, rows, HD), brief),
            pltpu.VMEM((3 * groups, heads, rows, HD), brief),
            pltpu.VMEM((2, groups, heads, rows), full),
            pltpu.VMEM((heads,) + matrices, full),
            pltpu.VMEM((groups, heads) + matrices, brief),
            pltpu.VMEM((groups, heads) + matrices, full),
            pltpu.VMEM((groups, heads) + matrices, full),
            pltpu.VMEM((groups, heads) + matrices, full),
            pltpu.VMEM((groups, heads) + matrices, full),
            pltpu.VMEM((heads,) + matrices, full),
            pltpu.VMEM((heads,) + matrices, full),
            pltpu.VMEM((2,) + matrices, full),
            pltpu.VMEM((2, span, tile, tile), full),
            pltpu.VMEM((moved, rows, HD), brief),
            pltpu.VMEM((moved, rows, HD), brief),
            pltpu.VMEM((moved, rows // HD, HD), full),
            dma((groups, heads, 3)),
            dma((4,)),
            dma((groups, heads, 2)),
            dma((groups, heads, 2)),
            dma((groups, heads, 2)),
            dma((groups, heads, 2)),
            dma((groups,)),
            dma((groups,)),
            dma((groups, heads)),
            dma((groups, heads)),
            dma((groups, heads)),
            dma((groups, heads)),
            dma((heads,)),
            dma((heads,)),
            dma((heads,)),
            dma((heads,)),
            dma((moved,)),
            dma((moved,)),
            dma((moved, 2)),
            dma((moved, 2)),
        ],
        compiler_params=pltpu.CompilerParams(
            collective_id=0, has_side_effects=True, vmem_limit_bytes=VMEM_GRANT
        ),
        name="whole_layer",
    )(queries, keys, values, rates, gate, up, down, steps, gain)
    return pl.pallas_call(
        functools.partial(finish_kernel, moved),
        in_specs=[pl.BlockSpec(memory_space=pltpu.VMEM)] * 7,
        out_specs=[pl.BlockSpec(memory_space=pltpu.HBM)] * 2,
        out_shape=[
            jax.ShapeDtypeStruct(queries.shape, brief),
            jax.ShapeDtypeStruct((3, heads, HD, width), full),
        ],
        scratch_shapes=[pltpu.VMEM((moved, rows, HD), brief), dma((3,)), dma((moved,))],
        compiler_params=pltpu.CompilerParams(vmem_limit_bytes=4 * 2**20),
        cost_estimate=pl.CostEstimate(
            flops=10 * moved * rows * HD,
            bytes_accessed=2 * groups * rows * features + 12 * heads * HD * width,
            transcendentals=2 * moved * rows * HD,
        ),
        name="finish_layer",
    )(*results)


def body(
    query_vectors,
    key_vectors,
    value_vectors,
    token_rates,
    gate_weight,
    up_weight,
    down_weight,
    step_sizes,
    norm_gain,
):
    group_count, tok_rows, feature_width = query_vectors.shape
    head_count = feature_width // HD
    rank = lax.axis_index("seq")
    count = lax.axis_size("seq")
    if count == 4 and group_count == 2 and head_count % 2 == 0:
        return whole_layer(
            query_vectors,
            key_vectors,
            value_vectors,
            token_rates,
            gate_weight,
            up_weight,
            down_weight,
            step_sizes,
            norm_gain[None, :],
        )
    swap = [(i, i ^ 1) for i in range(count)]
    ring = lambda d: [(i, (i + d) % count) for i in range(count)]
    shift = lambda a, route: lax.ppermute(a, "seq", route)
    odd = rank % 2 == 1

    far, near = [], []
    for group in range(group_count):
        far_pair, near_pair = [], []
        for tokens in (key_vectors, value_vectors):
            if group == 0:
                sent = tokens[0]
                route = [(i, i + 2) for i in range(count - 2)]
            else:
                sent = jnp.where(rank >= count - 2, tokens[group - 1], tokens[group])
                route = ring(2)
            far_block = shift(sent, route)
            far_pair.append(far_block)
            near_pair.append(shift(jnp.where(odd, far_block, tokens[group]), swap))
        far.append(far_pair)
        near.append(near_pair)

    spread = head_count == count
    first = jnp.stack([gate_weight, up_weight, down_weight], axis=1)
    rates = jnp.transpose(token_rates, (0, 2, 1))
    gain = norm_gain[None, :]
    bias = jnp.where(rank >= jnp.array([2, 1]), 0.0, EXCLUDED).astype(jnp.float32)
    pair_count = count // 2
    pair, core = rank // 2, rank % 2
    if spread:
        first_mine = lax.dynamic_slice_in_dim(first, rank, 1, 0)
        steps = lax.dynamic_slice_in_dim(step_sizes, rank, 1, 0)
    else:
        first_mine, steps = first, step_sizes
    weights_mine = first_mine
    low = first

    def gather(mine):
        arrived = [mine[0]] + [shift(mine[0], ring(2 * d)) for d in range(1, pair_count)]
        column = jnp.stack(arrived)
        other = shift(column, swap)
        blocks = []
        for head in range(head_count):
            at = (pair - head // 2) % pair_count
            pick = lambda a: lax.dynamic_index_in_dim(a, at, 0, keepdims=False)
            blocks.append(jnp.where(core == head % 2, pick(column), pick(other)))
        return blocks

    mixed = None
    for group in range(group_count):
        gradients = group_gradients(group, key_vectors, value_vectors, rates, low)
        last = group + 1 == group_count
        if spread:
            by_core = gradients.reshape((pair_count, 2) + gradients.shape[1:])
            kept = lax.dynamic_index_in_dim(by_core, core, 1, keepdims=False)
            given = lax.dynamic_index_in_dim(by_core, 1 - core, 1, keepdims=False)
            pair_sum = kept + shift(given, swap)
            block = lambda d: lax.dynamic_slice_in_dim(pair_sum, (pair + d) % pair_count, 1, 0)
            parts = [block(0)] + [shift(block(d), ring(2 * d)) for d in range(1, pair_count)]
        else:
            parts = [lax.psum(gradients, "seq")]
        mixed = mix(
            group,
            bias,
            query_vectors,
            (far[group][0], near[group][0]),
            (far[group][1], near[group][1]),
            key_vectors,
            value_vectors,
            low,
            gain,
            mixed,
        )
        weights_mine, low_mine = renew(parts, first_mine, weights_mine, steps)
        if not spread:
            low = low_mine
        elif not last:
            low = jnp.stack(gather(low_mine))
    if spread:
        final = jnp.stack(gather(weights_mine), axis=1)
    else:
        final = jnp.transpose(weights_mine, (1, 0, 2, 3))
    return (mixed, final)


def solution(mesh):
    return jax.shard_map(
        body,
        mesh=mesh,
        in_specs=(
            P("batch", "seq", "head"),
            P("batch", "seq", "head"),
            P("batch", "seq", "head"),
            P("batch", "head", "seq"),
            P("head", None, None),
            P("head", None, None),
            P("head", None, None),
            P("head"),
            P("head"),
        ),
        out_specs=(P("batch", "seq", "head"), P("batch", "head", None, None)),
        check_vma=False,
    )
```
